8 devices in a mesh: dp: 1 (over z), b: 2 (over y), a: 2 (over x), stage: 2 (over core).
Axes of the slice: x: 2, y: 2, z: 1, core: 2. Of those that a mesh axis runs over, the one named last changes fastest.
Arguments:
- embeds: bfloat16 [2, 6, 768, 4096], P('stage', 'dp')
- attn_gain: float32 [2, 4096], replicated
- w_query: bfloat16 [2, 4096, 4096], P(None, None, ('b', 'a'))
- w_key: bfloat16 [2, 4096, 1024], P(None, None, ('b', 'a'))
- w_value: bfloat16 [2, 4096, 1024], P(None, None, ('b', 'a'))
- w_out: bfloat16 [2, 4096, 4096], P(None, ('b', 'a'))
- mlp_gain: float32 [2, 4096], replicated
- w_gate: bfloat16 [2, 4096, 14336], P(None, None, ('b', 'a'))
- w_up: bfloat16 [2, 4096, 14336], P(None, None, ('b', 'a'))
- w_down: bfloat16 [2, 14336, 4096], P(None, ('b', 'a'))
Outputs:
- output 1: bfloat16 [2, 2, 6, 768, 8, 128], P('stage', None, ('dp', 'a'), None, 'b')
- output 2: bfloat16 [2, 2, 6, 768, 8, 128], P('stage', None, ('dp', 'a'), None, 'b')
- output 3: bfloat16 [2, 6, 4096], P('stage', ('dp', 'a'))
All inputs are finite; a program needn't handle non-finite values.
Results may differ from the reference program's by a relative error of at most 0.02.
Values are sent between devices in bfloat16 or wider.
A program may use at most 1 GiB of HBM per device.

```python
import jax
import jax.numpy as jnp
from jax import lax

MODEL_DIM = 4096
NUM_Q_HEADS = 32
NUM_KV_HEADS = 8
HEAD_DIM = 128
FFN_DIM = 14336
NUM_LAYERS = 2
REQUESTS = 6
SEQ_LEN = 768
ROPE_BASE = 500000.0
NORM_EPS = 1e-5


def setup_inputs(seed: int = 0, part: int = 0) -> dict:
    key_list = jax.random.split(jax.random.key(seed), 10)
    part_key = jax.random.fold_in(key_list[0], part)
    q_width = NUM_Q_HEADS * HEAD_DIM
    kv_width = NUM_KV_HEADS * HEAD_DIM
    out_scale = (SEQ_LEN ** 0.5 / 8.0) * q_width ** -0.5

    def draw_normal(rand_key, arr_shape, std_scale):
        return (jax.random.normal(rand_key, arr_shape, jnp.float32) * std_scale).astype(jnp.bfloat16)

    gain_pair = 1.0 + 0.2 * jax.random.normal(key_list[1], (2, NUM_LAYERS, MODEL_DIM), jnp.float32)
    return {
        'embeds': draw_normal(part_key, (2, REQUESTS, SEQ_LEN, MODEL_DIM), 1.0),
        'attn_gain': gain_pair[0],
        'w_query': draw_normal(key_list[2], (NUM_LAYERS, MODEL_DIM, q_width), MODEL_DIM ** -0.5),
        'w_key': draw_normal(key_list[3], (NUM_LAYERS, MODEL_DIM, kv_width), MODEL_DIM ** -0.5),
        'w_value': draw_normal(key_list[4], (NUM_LAYERS, MODEL_DIM, kv_width), MODEL_DIM ** -0.5),
        'w_out': draw_normal(key_list[5], (NUM_LAYERS, q_width, MODEL_DIM), out_scale),
        'mlp_gain': gain_pair[1],
        'w_gate': draw_normal(key_list[6], (NUM_LAYERS, MODEL_DIM, FFN_DIM), MODEL_DIM ** -0.5),
        'w_up': draw_normal(key_list[7], (NUM_LAYERS, MODEL_DIM, FFN_DIM), MODEL_DIM ** -0.5),
        'w_down': draw_normal(key_list[8], (NUM_LAYERS, FFN_DIM, MODEL_DIM), FFN_DIM ** -0.5),
    }


def rms_norm(hidden, gain_vec):
    as_f32 = hidden.astype(jnp.float32)
    inv_rms = lax.rsqrt(jnp.mean(as_f32 * as_f32, axis=-1, keepdims=True) + NORM_EPS)
    return (as_f32 * inv_rms * gain_vec).astype(jnp.bfloat16)


def rope_tables():
    half_dim = HEAD_DIM // 2
    inv_freq = ROPE_BASE ** (-2.0 * jnp.arange(half_dim, dtype=jnp.float32) / HEAD_DIM)
    angles = jnp.arange(SEQ_LEN, dtype=jnp.float32)[:, None] * inv_freq[None, :]
    return jnp.cos(angles), jnp.sin(angles)


def apply_rope(tensor, cos_t, sin_t):
    half_dim = HEAD_DIM // 2
    as_f32 = tensor.astype(jnp.float32)
    first_half = as_f32[..., :half_dim]
    second_half = as_f32[..., half_dim:]
    cos_b = cos_t[:, None, :]
    sin_b = sin_t[:, None, :]
    rotated = jnp.concatenate([first_half * cos_b - second_half * sin_b, second_half * cos_b + first_half * sin_b], axis=-1)
    return rotated.astype(jnp.bfloat16)


def attend_request(operands):
    q_one, k_one, v_one = operands
    group_size = NUM_Q_HEADS // NUM_KV_HEADS
    grouped = q_one.reshape(SEQ_LEN, NUM_KV_HEADS, group_size, HEAD_DIM).astype(jnp.float32)
    scores = jnp.einsum('qkgd,skd->kgqs', grouped, k_one.astype(jnp.float32)) * HEAD_DIM ** -0.5
    causal = jnp.arange(SEQ_LEN)[:, None] >= jnp.arange(SEQ_LEN)[None, :]
    scores = jnp.where(causal, scores, -1e30)
    attn_probs = jax.nn.softmax(scores, axis=-1).astype(jnp.bfloat16)
    attn_mix = jnp.einsum('kgqs,skd->qkgd', attn_probs.astype(jnp.float32), v_one.astype(jnp.float32))
    return attn_mix.astype(jnp.bfloat16).reshape(SEQ_LEN, NUM_Q_HEADS * HEAD_DIM)


def layer_step(hidden, layer_weights):
    attn_g, w_query, w_key, w_value, w_out, mlp_g, w_gate, w_up, w_down = layer_weights
    n_batch, seq_len, model_dim = hidden.shape
    cos_t, sin_t = rope_tables()
    normed = rms_norm(hidden, attn_g).reshape(n_batch * seq_len, model_dim)
    queries = jnp.dot(normed, w_query, preferred_element_type=jnp.float32).astype(jnp.bfloat16)
    queries = apply_rope(queries.reshape(n_batch, seq_len, NUM_Q_HEADS, HEAD_DIM), cos_t, sin_t)
    key_proj = jnp.dot(normed, w_key, preferred_element_type=jnp.float32).astype(jnp.bfloat16)
    key_rot = apply_rope(key_proj.reshape(n_batch, seq_len, NUM_KV_HEADS, HEAD_DIM), cos_t, sin_t)
    value_proj = jnp.dot(normed, w_value, preferred_element_type=jnp.float32).astype(jnp.bfloat16)
    value_proj = value_proj.reshape(n_batch, seq_len, NUM_KV_HEADS, HEAD_DIM)
    attn_mix = lax.map(attend_request, (queries, key_rot, value_proj))
    attn_out = jnp.dot(attn_mix.reshape(n_batch * seq_len, -1), w_out, preferred_element_type=jnp.float32).astype(jnp.bfloat16)
    hidden = hidden + attn_out.reshape(n_batch, seq_len, model_dim)
    normed = rms_norm(hidden, mlp_g).reshape(n_batch * seq_len, model_dim)
    gate_proj = jnp.dot(normed, w_gate, preferred_element_type=jnp.float32).astype(jnp.bfloat16)
    up_proj = jnp.dot(normed, w_up, preferred_element_type=jnp.float32).astype(jnp.bfloat16)
    activated = (jax.nn.silu(gate_proj.astype(jnp.float32)) * up_proj.astype(jnp.float32)).astype(jnp.bfloat16)
    mlp_out = jnp.dot(activated, w_down, preferred_element_type=jnp.float32).astype(jnp.bfloat16)
    hidden = hidden + mlp_out.reshape(n_batch, seq_len, model_dim)
    return hidden, (key_rot, value_proj)


def reference(embeds, attn_gain, w_query, w_key, w_value, w_out, mlp_gain, w_gate, w_up, w_down):
    final_hidden, cache_pair = lax.scan(layer_step, embeds[0], (attn_gain, w_query, w_key, w_value, w_out, mlp_gain, w_gate, w_up, w_down))
    key_stack, value_stack = cache_pair
    k_cache = jnp.stack([jnp.zeros_like(key_stack), key_stack])
    v_cache = jnp.stack([jnp.zeros_like(value_stack), value_stack])
    last_rows = final_hidden[:, SEQ_LEN - 1]
    last_hidden = jnp.stack([jnp.zeros_like(last_rows), last_rows])
    return k_cache, v_cache, last_hidden
```

```python
import functools

import jax
import jax.numpy as jnp
from jax import lax
from jax.experimental import pallas as pl
from jax.experimental.pallas import tpu as pltpu
from jax.sharding import PartitionSpec as P

HEAD_DIM = 128
ROPE_BASE = 500000.0
NORM_EPS = 1e-5
ALL_AXES = ('b', 'a', 'stage')
SWAP = [(0, 1), (1, 0)]
FROM_FAR = [(2, 1), (1, 3)]
FROM_NEAR = [(0, 1), (3, 3)]


def rms_norm(hidden, gain_vec):
    as_f32 = hidden.astype(jnp.float32)
    inv_rms = lax.rsqrt(jnp.mean(as_f32 * as_f32, axis=-1, keepdims=True) + NORM_EPS)
    return (as_f32 * inv_rms * gain_vec).astype(jnp.bfloat16)


def rope_tables(seq_len):
    half_dim = HEAD_DIM // 2
    inv_freq = ROPE_BASE ** (-2.0 * jnp.arange(half_dim, dtype=jnp.float32) / HEAD_DIM)
    angles = jnp.arange(seq_len, dtype=jnp.float32)[:, None] * inv_freq[None, :]
    cos_t, sin_t = jnp.cos(angles), jnp.sin(angles)
    return jnp.concatenate([cos_t, cos_t], axis=-1), jnp.concatenate([-sin_t, sin_t], axis=-1)


def matmul(left, right):
    return jnp.dot(left, right, preferred_element_type=jnp.float32)


def add_rounded(left, right):
    return (left.astype(jnp.float32) + right.astype(jnp.float32)).astype(jnp.bfloat16)


def rotate(as_f32, cos_rows, sin_rows):
    return (as_f32 * cos_rows + pltpu.roll(as_f32, HEAD_DIM // 2, 1) * sin_rows).astype(jnp.bfloat16)


def attention_kernel(q_block, group, _, q_ref, k_ref, v_ref, cos_ref, sin_ref, o_ref, kr_ref):
    step = pl.program_id(1)
    seq_len = k_ref.shape[0]

    @pl.when(step == 0)
    def _():
        kr_ref[...] = rotate(k_ref[...].astype(jnp.float32), cos_ref[...], sin_ref[...])

    for i in range(seq_len // q_block):
        @pl.when(step == i)
        def _(i=i):
            keys = min(seq_len, -(-(i + 1) * q_block // 128) * 128)
            rows = pl.ds(i * q_block, q_block)
            cos_rows, sin_rows = cos_ref[rows, :], sin_ref[rows, :]
            q = jnp.concatenate([
                rotate(q_ref[:, g * HEAD_DIM:(g + 1) * HEAD_DIM].astype(jnp.float32), cos_rows, sin_rows)
                for g in range(group)], axis=0)
            row = lax.rem(lax.broadcasted_iota(jnp.int32, (group * q_block, keys), 0), q_block) + i * q_block
            col = lax.broadcasted_iota(jnp.int32, (group * q_block, keys), 1)
            scores = lax.dot_general(q, kr_ref[:keys, :], (((1,), (1,)), ((), ())), preferred_element_type=jnp.float32)
            scores = jnp.where(row >= col, scores * HEAD_DIM ** -0.5, -1e30)
            probs = jnp.exp(scores - jnp.max(scores, axis=-1, keepdims=True))
            probs = probs * (1.0 / jnp.sum(probs, axis=-1, keepdims=True))
            mix = jnp.dot(probs.astype(jnp.bfloat16), v_ref[:keys, :], preferred_element_type=jnp.float32).astype(jnp.bfloat16)
            for g in range(group):
                o_ref[:, g * HEAD_DIM:(g + 1) * HEAD_DIM] = mix[g * q_block:(g + 1) * q_block]


def attention(q, k, v, cos_t, sin_t, order):
    seq_len, kv_width = k.shape
    q_block = seq_len // 8
    group = q.shape[1] // kv_width
    wide = group * HEAD_DIM
    return pl.pallas_call(
        functools.partial(attention_kernel, q_block, group),
        grid_spec=pltpu.PrefetchScalarGridSpec(
            num_scalar_prefetch=1,
            grid=(kv_width // HEAD_DIM, 8),
            in_specs=[
                pl.BlockSpec((q_block, wide), lambda h, i, order_ref: (i, h)),
                pl.BlockSpec((seq_len, HEAD_DIM), lambda h, i, order_ref: (0, h)),
                pl.BlockSpec((seq_len, HEAD_DIM), lambda h, i, order_ref: (0, h)),
                pl.BlockSpec((seq_len, HEAD_DIM), lambda h, i, order_ref: (0, 0)),
                pl.BlockSpec((seq_len, HEAD_DIM), lambda h, i, order_ref: (0, 0)),
            ],
            out_specs=[
                pl.BlockSpec((q_block, wide), lambda h, i, order_ref: (order_ref[i], h)),
                pl.BlockSpec((seq_len, HEAD_DIM), lambda h, i, order_ref: (0, h)),
            ],
        ),
        out_shape=[jax.ShapeDtypeStruct(q.shape, jnp.bfloat16), jax.ShapeDtypeStruct(k.shape, jnp.bfloat16)],
        compiler_params=pltpu.CompilerParams(vmem_limit_bytes=32 * 1024 * 1024),
        cost_estimate=pl.CostEstimate(flops=9_000_000_000, bytes_accessed=5_000_000, transcendentals=4_000_000),
    )(order, q, k, v, cos_t, sin_t)


def kv_kernel(part_ref, x_ref, gain_ref, mine_ref, other_ref, cos_ref, sin_ref, o_ref, normed):
    step = pl.program_id(0)
    half = mine_ref.shape[0]

    @pl.when(step == 0)
    def _():
        as_f32 = x_ref[...].astype(jnp.float32)
        inv_rms = lax.rsqrt(jnp.mean(as_f32 * as_f32, axis=-1, keepdims=True) + NORM_EPS)
        whole = (as_f32 * inv_rms * gain_ref[...]).astype(jnp.bfloat16)
        normed[0] = whole[:, :half]
        normed[1] = whole[:, half:]

    part = part_ref[0]
    product = jnp.dot(normed[part], mine_ref[...], preferred_element_type=jnp.float32)
    product += jnp.dot(normed[1 - part], other_ref[...], preferred_element_type=jnp.float32)
    rounded = product.astype(jnp.bfloat16)

    @pl.when(step % 2 == 0)
    def _():
        for h in range(rounded.shape[1] // HEAD_DIM):
            cols = slice(h * HEAD_DIM, (h + 1) * HEAD_DIM)
            o_ref[:, cols] = rotate(rounded[:, cols].astype(jnp.float32), cos_ref[...], sin_ref[...])

    @pl.when(step % 2 == 1)
    def _():
        o_ref[...] = rounded


def keys_values(x, gain, mine, other, cos_rows, sin_rows, part, tile):
    rows, width = x.shape
    half, columns = mine.shape
    return pl.pallas_call(
        kv_kernel,
        grid_spec=pltpu.PrefetchScalarGridSpec(
            num_scalar_prefetch=1,
            grid=(columns // tile,),
            in_specs=[
                pl.BlockSpec((rows, width), lambda j, part_ref: (0, 0)),
                pl.BlockSpec((1, width), lambda j, part_ref: (0, 0)),
                pl.BlockSpec((half, tile), lambda j, part_ref: (0, j)),
                pl.BlockSpec((half, tile), lambda j, part_ref: (0, j)),
                pl.BlockSpec((rows, HEAD_DIM), lambda j, part_ref: (0, 0)),
                pl.BlockSpec((rows, HEAD_DIM), lambda j, part_ref: (0, 0)),
            ],
            out_specs=pl.BlockSpec((rows, tile), lambda j, part_ref: (0, j)),
            scratch_shapes=[pltpu.VMEM((2, rows, half), jnp.bfloat16)],
        ),
        out_shape=jax.ShapeDtypeStruct((rows, columns), jnp.bfloat16),
        compiler_params=pltpu.CompilerParams(vmem_limit_bytes=32 * 1024 * 1024),
        cost_estimate=pl.CostEstimate(flops=4 * rows * half * columns, bytes_accessed=4 * half * columns, transcendentals=0),
    )(part, x, gain, mine, other, cos_rows, sin_rows)


def last_attention_kernel(n_chunk, kv_heads, order_ref, q_ref, cos_ref, sin_ref, *refs):
    kv_refs, o_ref = refs[:n_chunk], refs[n_chunk]
    kv_width = kv_heads * HEAD_DIM
    group = q_ref.shape[2]
    low_lanes = lax.broadcasted_iota(jnp.int32, (group, HEAD_DIM), 1) < HEAD_DIM // 2
    for c in range(n_chunk):
        for piece in range(4):
            for h in range(kv_heads):
                head = order_ref[piece] * kv_heads + h
                q = rotate(q_ref[head, order_ref[4] + c].astype(jnp.float32), cos_ref[...], sin_ref[...])
                low = 2 * piece * kv_width + h * HEAD_DIM
                k = kv_refs[c][:, low:low + HEAD_DIM]
                v = kv_refs[c][:, low + kv_width:low + kv_width + HEAD_DIM]
                scores = lax.dot_general(q, k, (((1,), (1,)), ((), ())), preferred_element_type=jnp.float32) * HEAD_DIM ** -0.5
                top = jnp.max(scores, axis=-1, keepdims=True)
                probs = jnp.exp(scores - top)
                total = jnp.sum(probs, axis=-1, keepdims=True)
                o_ref[c, head, :, :HEAD_DIM] = jnp.dot(probs.astype(jnp.bfloat16), v, preferred_element_type=jnp.float32)
                o_ref[c, head, :, HEAD_DIM:] = jnp.where(low_lanes, top, total)


def last_attention(q_all, cos_row, sin_row, kv_list, kv_heads, order):
    n_chunk = len(kv_list)
    heads, group = q_all.shape[0], q_all.shape[2]
    vmem = pl.BlockSpec(memory_space=pltpu.VMEM)
    return pl.pallas_call(
        functools.partial(last_attention_kernel, n_chunk, kv_heads),
        in_specs=[pl.BlockSpec(memory_space=pltpu.SMEM)] + [vmem] * (3 + n_chunk),
        out_specs=vmem,
        out_shape=jax.ShapeDtypeStruct((n_chunk, heads, group, 2 * HEAD_DIM), jnp.float32),
        compiler_params=pltpu.CompilerParams(vmem_limit_bytes=32 * 1024 * 1024),
        cost_estimate=pl.CostEstimate(flops=1_000_000_000, bytes_accessed=3_000_000, transcendentals=0),
    )(order, q_all, cos_row, sin_row, *kv_list)


def row_kernel(has_gain, has_two, _, x_ref, *refs):
    rows = x_ref[...]
    if has_gain:
        gain_ref, refs = refs[0], refs[1:]
        as_f32 = rows.astype(jnp.float32)
        inv_rms = lax.rsqrt(jnp.mean(as_f32 * as_f32, axis=-1, keepdims=True) + NORM_EPS)
        rows = (as_f32 * inv_rms * gain_ref[...]).astype(jnp.bfloat16)
    product = jnp.dot(rows, refs[0][0], preferred_element_type=jnp.float32)
    if has_two:
        gate = product.astype(jnp.bfloat16).astype(jnp.float32)
        up = jnp.dot(rows, refs[1][0], preferred_element_type=jnp.float32).astype(jnp.bfloat16).astype(jnp.float32)
        product = gate * (1.0 / (1.0 + jnp.exp(-gate))) * up
    o_ref = refs[-1]
    o_ref[...] = product.astype(o_ref.dtype)


def row_product(rows, gain, weights, layer, part, by_columns, tile, dtype):
    n_rows = rows.shape[0]
    depth, width = weights[0].shape[1:]
    if by_columns:
        width //= 2
        tiles = width // tile
        w_spec = pl.BlockSpec((1, depth, tile), lambda j, part_ref: (layer, 0, part_ref[0] * tiles + j))
    else:
        depth //= 2
        tiles = width // tile
        w_spec = pl.BlockSpec((1, depth, tile), lambda j, part_ref: (layer, part_ref[0], j))
    gains = [] if gain is None else [gain]
    return pl.pallas_call(
        functools.partial(row_kernel, gain is not None, len(weights) == 2),
        grid_spec=pltpu.PrefetchScalarGridSpec(
            num_scalar_prefetch=1,
            grid=(tiles,),
            in_specs=[pl.BlockSpec((n_rows, depth), lambda j, part_ref: (0, 0))]
            + [pl.BlockSpec((1, depth), lambda j, part_ref: (0, 0))] * len(gains) + [w_spec] * len(weights),
            out_specs=pl.BlockSpec((n_rows, tile), lambda j, part_ref: (0, j)),
        ),
        out_shape=jax.ShapeDtypeStruct((n_rows, width), dtype),
        compiler_params=pltpu.CompilerParams(vmem_limit_bytes=40 * 1024 * 1024),
        cost_estimate=pl.CostEstimate(flops=200 * depth * width, bytes_accessed=2 * depth * width, transcendentals=0),
    )(part, rows, *gains, *weights)


def first_cut_kernel(where_ref, near_ref, far_ref, k_ref, v_ref):
    kv_width = near_ref.shape[-1] // 2
    own_low = where_ref[0] == 0
    near, far = near_ref[0], far_ref[0]
    low, high = jnp.where(own_low, near, far), jnp.where(own_low, far, near)
    k_ref[0, 0, :, :kv_width] = low[:, :kv_width]
    k_ref[0, 0, :, kv_width:] = high[:, :kv_width]
    v_ref[0, 0, :, :kv_width] = low[:, kv_width:]
    v_ref[0, 0, :, kv_width:] = high[:, kv_width:]


def first_cut(near, far, where):
    n_chunk, seq_len, columns = near.shape
    rows = seq_len // 2
    source = pl.BlockSpec((1, rows, columns), lambda c, j, where_ref: (c, j, 0))
    target = pl.BlockSpec((1, 1, rows, columns), lambda c, j, where_ref: (0, c, j, 0))
    return pl.pallas_call(
        first_cut_kernel,
        grid_spec=pltpu.PrefetchScalarGridSpec(num_scalar_prefetch=1, grid=(n_chunk, 2), in_specs=[source] * 2, out_specs=[target] * 2),
        out_shape=[jax.ShapeDtypeStruct((2, n_chunk, seq_len, columns), jnp.bfloat16)] * 2,
        compiler_params=pltpu.CompilerParams(vmem_limit_bytes=32 * 1024 * 1024),
        cost_estimate=pl.CostEstimate(flops=1_000_000_000, bytes_accessed=19_000_000, transcendentals=0),
    )(where, near, far)


def second_cut_kernel(where_ref, near_ref, far_ref, k_in, v_in, k_ref, v_ref):
    columns = near_ref.shape[-1] // 2
    kv_width = columns // 2

    def put(source):
        mine, other = source[:, :columns], source[:, columns:]
        own_low = where_ref[0] + pl.program_id(0) - 2 * where_ref[0] * pl.program_id(0) == 0
        low, high = jnp.where(own_low, mine, other), jnp.where(own_low, other, mine)
        k_ref[0, 0, :, :kv_width] = low[:, :kv_width]
        k_ref[0, 0, :, kv_width:] = high[:, :kv_width]
        v_ref[0, 0, :, :kv_width] = low[:, kv_width:]
        v_ref[0, 0, :, kv_width:] = high[:, kv_width:]

    @pl.when(pl.program_id(0) == 0)
    def _():
        put(near_ref[0])

    @pl.when(pl.program_id(0) == 1)
    def _():
        put(far_ref[0])


def second_cut(near, far, where, k_flat, v_flat, request):
    _, rows, columns = near.shape
    block = rows // 2

    def place(i, j, half, where_ref):
        along_x = where_ref[0] + i - 2 * where_ref[0] * i
        along_y = where_ref[1] + j - 2 * where_ref[1] * j
        return 1, request, (1 - half) * (2 * along_x + along_y) + half * (4 + 2 * along_y + along_x), 0

    source = pl.BlockSpec((1, block, columns), lambda i, j, half, where_ref: (j, half, 0))
    target = pl.BlockSpec((1, 1, block, columns // 2), place)
    whole = pl.BlockSpec(memory_space=pl.ANY)
    return pl.pallas_call(
        second_cut_kernel,
        grid_spec=pltpu.PrefetchScalarGridSpec(
            num_scalar_prefetch=1, grid=(2, 2, 2), in_specs=[source] * 2 + [whole] * 2, out_specs=[target] * 2),
        out_shape=[jax.ShapeDtypeStruct(k_flat.shape, jnp.bfloat16)] * 2,
        input_output_aliases={3: 0, 4: 1},
        compiler_params=pltpu.CompilerParams(vmem_limit_bytes=32 * 1024 * 1024),
        cost_estimate=pl.CostEstimate(flops=300_000_000, bytes_accessed=5_000_000, transcendentals=0),
    )(where, near, far, k_flat, v_flat)


def solution(mesh):
    tp_axes = ('b', 'a')
    weight_cols = P(None, None, tp_axes)
    weight_rows = P(None, tp_axes, None)
    in_specs = (P('stage', 'dp', None, None), P(), weight_cols, weight_cols, weight_cols, weight_rows, P(), weight_cols, weight_cols, weight_rows)
    cache_spec = P('stage', None, ('dp', 'a'), None, 'b', None)
    out_specs = (cache_spec, cache_spec, P('stage', ('dp', 'a'), None))

    def over_x(value):
        return lax.ppermute(value, 'a', SWAP)

    def over_y(value):
        return lax.ppermute(value, 'b', SWAP)

    def across(value):
        return lax.ppermute(value, 'stage', SWAP)

    def hold(values, *after):
        return lax.optimization_barrier((values, after))[0]

    def stage_body(embeds, attn_gain, w_query, w_key, w_value, w_out, mlp_gain, w_gate, w_up, w_down):
        a, b, s = lax.axis_index('a'), lax.axis_index('b'), lax.axis_index('stage')
        n_req, seq_len, width = embeds.shape[1:]
        n_chunk = n_req // 2
        block = seq_len // 8
        kv_width = w_key.shape[2]
        kv_heads = kv_width // HEAD_DIM
        kv2 = 2 * kv_width
        half_rows = seq_len // 2
        half_width = width // 2
        cos_t, sin_t = rope_tables(seq_len)
        chip = 2 * b + a
        part = s.astype(jnp.int32).reshape(1)
        where = jnp.stack([a, b]).astype(jnp.int32)

        fours = jnp.arange(4, dtype=jnp.int32)
        order = jnp.concatenate([jnp.bitwise_xor(fours, 2 * a + b), 4 + jnp.bitwise_xor(fours, chip)]).astype(jnp.int32)

        def own_rows(value):
            return jnp.concatenate([
                lax.dynamic_slice_in_dim(value, block * (2 * a + b), block, 0),
                lax.dynamic_slice_in_dim(value, half_rows + block * chip, block, 0)], axis=0)

        def send_parts(part_sum):
            quarter = 2 * block
            return part_sum[quarter:2 * quarter], part_sum[3 * quarter:]

        def send_wide(sends):
            return over_x(sends[0]), over_y(sends[1])

        def add_wide(part_sum, got):
            quarter = 2 * block
            return add_rounded(part_sum[:quarter], got[0]), add_rounded(part_sum[2 * quarter:3 * quarter], got[1])

        def send_narrow(sums):
            return over_y(sums[0][block:]), over_x(sums[1][block:])

        def add_narrow(residual, sums, got):
            kept = jnp.concatenate([sums[0][:block], sums[1][:block]], axis=0)
            return add_rounded(residual, add_rounded(kept, jnp.concatenate(got, axis=0)))

        def gather_near(own):
            return over_y(own[:block]), over_x(own[block:])

        def join_near(own, got):
            return jnp.concatenate([own[:block], got[0]], axis=0), jnp.concatenate([own[block:], got[1]], axis=0)

        def gather_far(near):
            return over_x(near[0]), over_y(near[1])

        def join_far(near, far):
            return jnp.concatenate([near[0], far[0], near[1], far[1]], axis=0)

        moved = []
        for c in range(n_chunk):
            moved.append(lax.ppermute(embeds[0, n_chunk + c], 'stage', [(0, 1)]))

        w_kv = jnp.concatenate([w_key[1], w_value[1]], axis=1)
        w_mine = lax.dynamic_slice_in_dim(w_kv, s * half_width, half_width, 0)
        top, bottom = w_mine[:width // 4], w_mine[width // 4:]
        top_y = over_y(top)
        bottom_x = over_x(bottom)

        def project(x):
            normed = rms_norm(x, attn_gain[0])
            q = matmul(normed, w_query[0]).astype(jnp.bfloat16)
            k = matmul(normed, w_key[0]).astype(jnp.bfloat16)
            v = matmul(normed, w_value[0]).astype(jnp.bfloat16)
            return q, k, v

        def attend(q, k, v):
            mix, k_rot = attention(q, k, v, cos_t, sin_t, order)
            return matmul(mix, w_out[0]).astype(jnp.bfloat16), jnp.concatenate([k_rot, v], axis=1)

        def gate_of(normed):
            return matmul(normed, w_gate[0]).astype(jnp.bfloat16)

        def act_of(normed, gate):
            up = matmul(normed, w_up[0]).astype(jnp.bfloat16)
            return (jax.nn.silu(gate.astype(jnp.float32)) * up.astype(jnp.float32)).astype(jnp.bfloat16)

        def down_of(act):
            return matmul(act, w_down[0]).astype(jnp.bfloat16)

        def hidden_of(c, first, second):
            return jnp.where(s == 0, first, second)

        own_cos, own_sin = own_rows(cos_t), own_rows(sin_t)

        x0 = hidden_of(0, embeds[0, 0], moved[0])
        qkv0 = project(x0)
        top_y, bottom_x = hold((top_y, bottom_x), qkv0)
        top_xd = over_x(jnp.concatenate([top, top_y], axis=1))
        bottom_yd = over_y(jnp.concatenate([bottom, bottom_x], axis=1))
        p0, kv0_0 = attend(*qkv0)
        own_x0 = own_rows(x0)
        send = send_parts(p0)
        wide0 = send_wide(send)

        x1 = hidden_of(1, *hold((embeds[0, 1], moved[1]), send))
        p1, kv0_1 = attend(*project(x1))
        own_x1 = own_rows(x1)
        send = send_parts(p1)
        wide1 = send_wide(send)

        sums0 = add_wide(p0, hold(wide0, send))
        narrow0 = send_narrow(sums0)

        x2 = hidden_of(2, *hold((embeds[0, 2], moved[2]), sums0))
        p2, kv0_2 = attend(*project(x2))
        own_x2 = own_rows(x2)

        sums1 = add_wide(p1, hold(wide1, p2))
        narrow1 = send_narrow(sums1)
        own1_0 = add_narrow(own_x0, sums0, hold(narrow0, sums1))
        h0 = rms_norm(own1_0, mlp_gain[0])
        near_got0 = gather_near(h0)

        top_xd, bottom_yd = hold((top_xd, bottom_yd), h0)
        w_half = jnp.concatenate([
            jnp.concatenate([top, top_xd[:, :kv2], top_y, top_xd[:, kv2:]], axis=1),
            jnp.concatenate([bottom, bottom_x, bottom_yd[:, :kv2], bottom_yd[:, kv2:]], axis=1)], axis=0)
        w_other = across(w_half)

        own1_1 = add_narrow(own_x1, sums1, hold(narrow1, w_half))
        h1 = rms_norm(own1_1, mlp_gain[0])
        near_got1 = gather_near(h1)
        near0 = join_near(h0, hold(near_got0, h1))
        far0 = gather_far(near0)
        send = hold(send_parts(p2), near0)
        wide2 = send_wide(send)
        near1 = join_near(h1, hold(near_got1, send))
        far1 = gather_far(near1)

        normed = join_far(near0, hold(far0, near1))
        act = act_of(normed, gate_of(normed))
        sums2 = add_wide(p2, hold(wide2, act))
        narrow2 = send_narrow(sums2)
        d0 = down_of(hold(act, sums2))
        send = send_parts(d0)
        wide0 = send_wide(send)

        normed = join_far(near1, hold(far1, send))
        gate = gate_of(normed)
        own1_2 = add_narrow(own_x2, sums2, hold(narrow2, gate))
        h2 = rms_norm(own1_2, mlp_gain[0])
        near_got2 = gather_near(h2)
        act = act_of(hold(normed, h2), gate)
        sums0 = add_wide(d0, hold(wide0, act))
        narrow0 = send_narrow(sums0)
        near2 = join_near(h2, hold(near_got2, sums0))
        far2 = gather_far(near2)
        d1 = down_of(hold(act, near2))
        send = send_parts(d1)
        wide1 = send_wide(send)

        def keys_values_of(final):
            return keys_values(final, attn_gain[1:2], w_half, w_other, own_cos, own_sin, part, kv_width)

        def to_decode(value):
            return lax.ppermute(value, ('a', 'stage'), FROM_NEAR), lax.ppermute(value, ('a', 'stage'), FROM_FAR)

        final0 = add_narrow(own1_0, sums0, hold(narrow0, send))
        kv1_0 = keys_values_of(final0)
        cut0 = to_decode(hold(jnp.stack([kv0_0, kv0_1, kv0_2]), kv1_0))

        normed = join_far(near2, hold(far2, kv1_0))
        gate = gate_of(normed)
        act = act_of(normed, gate)
        sums1 = add_wide(d1, hold(wide1, act))
        narrow1 = send_narrow(sums1)
        d2 = down_of(hold(act, sums1))
        send = send_parts(d2)
        wide2 = send_wide(send)
        final1 = add_narrow(own1_1, sums1, hold(narrow1, send))
        kv1_1 = keys_values_of(final1)
        k_flat, v_flat = first_cut(*hold(cut0, kv1_1), where)
        sums2 = add_wide(d2, hold(wide2, k_flat))
        narrow2 = send_narrow(sums2)

        def along_y(kv, *after):
            return over_y(hold(kv[:, 2 * kv2:], *after))

        def to_decode_rows(kv, got):
            return to_decode(jnp.stack([kv[:, :2 * kv2], got]))

        got_0 = along_y(kv1_0, sums2)
        got_1 = along_y(kv1_1, sums2)

        final2 = add_narrow(own1_2, sums2, narrow2)
        last_own = jnp.concatenate([f[2 * block - 1:] for f in (final0, final1, final2)], axis=0)
        everyone = lax.all_gather(last_own, ALL_AXES, axis=0)
        last = everyone[6:8].reshape(n_req, width)

        def pad_rows(value):
            return jnp.pad(value, ((0, 16 - n_req), (0, 0)))

        q_part = row_product(pad_rows(last), attn_gain[1:2], [w_query], 1, part, True, kv_width, jnp.bfloat16)
        kv1_2 = keys_values_of(hold(final2, q_part))
        q_all = lax.all_gather(q_part[:n_req].reshape(n_req, -1, HEAD_DIM), ALL_AXES, axis=0)
        chips = jnp.stack([chip, chip + 1 - 2 * a, chip + 2 - 4 * b, 3 - chip, s * n_chunk]).astype(jnp.int32)
        packed = last_attention(q_all, cos_t[-1:], sin_t[-1:], [kv1_0, kv1_1, kv1_2], kv_heads, chips)
        gathered = lax.all_gather(packed, ALL_AXES, axis=0)
        got_2 = along_y(kv1_2, gathered)
        cut1_0 = to_decode_rows(hold(kv1_0, gathered), hold(got_0, gathered))
        cut1_1 = to_decode_rows(hold(kv1_1, gathered), hold(got_1, gathered))

        heads = gathered.reshape((4, 2) + packed.shape)
        mine = lax.dynamic_index_in_dim(heads, 2 * chip + s, 3, keepdims=False)
        tops = mine[..., HEAD_DIM:HEAD_DIM + 1]
        totals = mine[..., 2 * HEAD_DIM - 1:]
        scale = jnp.exp(tops - jnp.max(tops, axis=0, keepdims=True))
        attn_mine = jnp.sum(mine[..., :HEAD_DIM] * scale, axis=0) / jnp.sum(totals * scale, axis=0)
        attn_mine = pad_rows(attn_mine.astype(jnp.bfloat16).reshape(n_req, -1))
        out_part = row_product(attn_mine, None, [w_out], 1, part, False, 1024, jnp.float32)
        out_all = lax.all_gather(out_part[:n_req], ALL_AXES, axis=0)
        cut1_2 = to_decode_rows(hold(kv1_2, out_all), hold(got_2, out_all))
        last = add_rounded(last, jnp.sum(out_all, axis=0).astype(jnp.bfloat16))
        act_last = row_product(pad_rows(last), mlp_gain[1:2], [w_gate, w_up], 1, part, True, 256, jnp.bfloat16)
        down_part = row_product(act_last, None, [w_down], 1, part, False, 512, jnp.float32)
        down_all = lax.all_gather(down_part[:n_req], ALL_AXES, axis=0)
        last = add_rounded(last, jnp.sum(down_all, axis=0).astype(jnp.bfloat16))
        last_out = lax.dynamic_slice_in_dim(last, a * n_chunk, n_chunk, 0)
        last_out = jnp.where(s == 1, last_out, jnp.zeros_like(last_out))

        for c, cut in enumerate((cut1_0, cut1_1, cut1_2)):
            k_flat, v_flat = second_cut(*cut, where, k_flat, v_flat, c)
        cache_shape = (1, 2, n_chunk, seq_len, 2 * kv_heads, HEAD_DIM)
        return k_flat.reshape(cache_shape), v_flat.reshape(cache_shape), last_out[None]

    return jax.shard_map(stage_body, mesh=mesh, in_specs=in_specs, out_specs=out_specs, check_vma=False)
```

```python
import functools

import jax
import jax.numpy as jnp
from jax import lax
from jax.experimental import pallas as pl
from jax.experimental.pallas import tpu as pltpu
from jax.sharding import PartitionSpec as P


HEAD_DIM = 128
ROPE_BASE = 500000.0
NORM_EPS = 1e-5
SWAP = [(0, 1), (1, 0)]
FROM_FAR = [(2, 1), (1, 3)]
FROM_NEAR = [(0, 1), (3, 3)]


def rms_norm(hidden, gain_vec):
    as_f32 = hidden.astype(jnp.float32)
    inv_rms = lax.rsqrt(jnp.mean(as_f32 * as_f32, axis=-1, keepdims=True) + NORM_EPS)
    return (as_f32 * inv_rms * gain_vec).astype(jnp.bfloat16)


def rope_tables(seq_len):
    half_dim = HEAD_DIM // 2
    inv_freq = ROPE_BASE ** (-2.0 * jnp.arange(half_dim, dtype=jnp.float32) / HEAD_DIM)
    angles = jnp.arange(seq_len, dtype=jnp.float32)[:, None] * inv_freq[None, :]
    cos_t, sin_t = jnp.cos(angles), jnp.sin(angles)
    return jnp.concatenate([cos_t, cos_t], axis=-1), jnp.concatenate([-sin_t, sin_t], axis=-1)


def matmul(left, right):
    return jnp.dot(left, right, preferred_element_type=jnp.float32)


def add_rounded(left, right):
    return (left.astype(jnp.float32) + right.astype(jnp.float32)).astype(jnp.bfloat16)


def rotate(as_f32, cos_rows, sin_rows):
    return (as_f32 * cos_rows + pltpu.roll(as_f32, HEAD_DIM // 2, 1) * sin_rows).astype(jnp.bfloat16)


def attention_kernel(q_block, group, _, q_ref, k_ref, v_ref, cos_ref, sin_ref, o_ref, kr_ref):
    step = pl.program_id(1)
    seq_len = k_ref.shape[0]

    @pl.when(step == 0)
    def _():
        kr_ref[...] = rotate(k_ref[...].astype(jnp.float32), cos_ref[...], sin_ref[...])

    for i in range(seq_len // q_block):
        @pl.when(step == i)
        def _(i=i):
            keys = min(seq_len, -(-(i + 1) * q_block // 128) * 128)
            rows = pl.ds(i * q_block, q_block)
            cos_rows, sin_rows = cos_ref[rows, :], sin_ref[rows, :]
            q = jnp.concatenate([
                rotate(q_ref[:, g * HEAD_DIM:(g + 1) * HEAD_DIM].astype(jnp.float32), cos_rows, sin_rows)
                for g in range(group)], axis=0)
            row = lax.rem(lax.broadcasted_iota(jnp.int32, (group * q_block, keys), 0), q_block) + i * q_block
            col = lax.broadcasted_iota(jnp.int32, (group * q_block, keys), 1)
            scores = lax.dot_general(q, kr_ref[:keys, :], (((1,), (1,)), ((), ())), preferred_element_type=jnp.float32)
            scores = jnp.where(row >= col, scores * HEAD_DIM ** -0.5, -1e30)
            probs = jnp.exp(scores - jnp.max(scores, axis=-1, keepdims=True))
            probs = probs * (1.0 / jnp.sum(probs, axis=-1, keepdims=True))
            mix = jnp.dot(probs.astype(jnp.bfloat16), v_ref[:keys, :], preferred_element_type=jnp.float32).astype(jnp.bfloat16)
            for g in range(group):
                o_ref[:, g * HEAD_DIM:(g + 1) * HEAD_DIM] = mix[g * q_block:(g + 1) * q_block]


def attention(q, k, v, cos_t, sin_t, order):
    seq_len, kv_width = k.shape
    q_block = seq_len // 8
    group = q.shape[1] // kv_width
    wide = group * HEAD_DIM
    return pl.pallas_call(
        functools.partial(attention_kernel, q_block, group),
        grid_spec=pltpu.PrefetchScalarGridSpec(
            num_scalar_prefetch=1,
            grid=(kv_width // HEAD_DIM, 8),
            in_specs=[
                pl.BlockSpec((q_block, wide), lambda h, i, order_ref: (i, h)),
                pl.BlockSpec((seq_len, HEAD_DIM), lambda h, i, order_ref: (0, h)),
                pl.BlockSpec((seq_len, HEAD_DIM), lambda h, i, order_ref: (0, h)),
                pl.BlockSpec((seq_len, HEAD_DIM), lambda h, i, order_ref: (0, 0)),
                pl.BlockSpec((seq_len, HEAD_DIM), lambda h, i, order_ref: (0, 0)),
            ],
            out_specs=[
                pl.BlockSpec((q_block, wide), lambda h, i, order_ref: (order_ref[i], h)),
                pl.BlockSpec((seq_len, HEAD_DIM), lambda h, i, order_ref: (0, h)),
            ],
        ),
        out_shape=[jax.ShapeDtypeStruct(q.shape, jnp.bfloat16), jax.ShapeDtypeStruct(k.shape, jnp.bfloat16)],
        compiler_params=pltpu.CompilerParams(vmem_limit_bytes=32 * 1024 * 1024),
        cost_estimate=pl.CostEstimate(flops=9_000_000_000, bytes_accessed=5_000_000, transcendentals=4_000_000),
    )(order, q, k, v, cos_t, sin_t)


def kv_kernel(part_ref, x_ref, gain_ref, cos_ref, sin_ref, *refs):
    mine, other, o_ref, normed = refs[:8], refs[8:16], refs[16], refs[17]
    depth, columns = mine[0].shape
    half = 2 * depth
    as_f32 = x_ref[...].astype(jnp.float32)
    inv_rms = lax.rsqrt(jnp.mean(as_f32 * as_f32, axis=-1, keepdims=True) + NORM_EPS)
    whole = (as_f32 * inv_rms * gain_ref[...]).astype(jnp.bfloat16)
    normed[0] = whole[:, :half]
    normed[1] = whole[:, half:]
    part = part_ref[0]
    for piece in range(4):
        product = jnp.dot(normed[part, :, :depth], mine[2 * piece][...], preferred_element_type=jnp.float32)
        product += jnp.dot(normed[part, :, depth:], mine[2 * piece + 1][...], preferred_element_type=jnp.float32)
        product += jnp.dot(normed[1 - part, :, :depth], other[2 * piece][...], preferred_element_type=jnp.float32)
        product += jnp.dot(normed[1 - part, :, depth:], other[2 * piece + 1][...], preferred_element_type=jnp.float32)
        rounded = product.astype(jnp.bfloat16)
        base = piece * columns
        for h in range(columns // 2 // HEAD_DIM):
            cols = slice(h * HEAD_DIM, (h + 1) * HEAD_DIM)
            o_ref[:, base + h * HEAD_DIM:base + (h + 1) * HEAD_DIM] = rotate(rounded[:, cols].astype(jnp.float32), cos_ref[...], sin_ref[...])
        o_ref[:, base + columns // 2:base + columns] = rounded[:, columns // 2:]


def keys_values(x, gain, mine, other, cos_rows, sin_rows, part):
    rows, _ = x.shape
    depth, columns = mine[0].shape
    vmem = pl.BlockSpec(memory_space=pltpu.VMEM)
    return pl.pallas_call(
        kv_kernel,
        in_specs=[pl.BlockSpec(memory_space=pltpu.SMEM)] + [vmem] * 20,
        out_specs=vmem,
        out_shape=jax.ShapeDtypeStruct((rows, 4 * columns), jnp.bfloat16),
        scratch_shapes=[pltpu.VMEM((2, rows, 2 * depth), jnp.bfloat16)],
        compiler_params=pltpu.CompilerParams(vmem_limit_bytes=40 * 1024 * 1024),
        cost_estimate=pl.CostEstimate(flops=32 * rows * depth * columns, bytes_accessed=32 * depth * columns, transcendentals=0),
    )(part, x, gain, cos_rows, sin_rows, *mine, *other)


def tail_kernel(kv_heads, x0_ref, x1_ref, x2_ref, kv0_ref, kv1_ref, kv2_ref, gain_a_ref, gain_m_ref, cos_ref, sin_ref,
                wq_hbm, wo_hbm, wg_hbm, wu_hbm, wd_hbm, o_ref,
                wq, wo, wg, wu, wd, x_src, x_all, q_src, q_all, pk_src, pk_all, mix, p_src, p_all, r_src, r_all,
                w_sem, x_send, x_recv, q_send, q_recv, pk_send, pk_recv, p_send, p_recv, r_send, r_recv):
    a, b, s = lax.axis_index('a'), lax.axis_index('b'), lax.axis_index('stage')
    me = 4 * b + 2 * a + s
    x_refs, kv_refs = (x0_ref, x1_ref, x2_ref), (kv0_ref, kv1_ref, kv2_ref)
    n_chunk = len(x_refs)
    n_rows = o_ref.shape[0]
    group = wq.shape[1] // HEAD_DIM
    eighth, wide = wq.shape[1], wg.shape[1]

    cuts = [
        (wq_hbm.at[1, :, pl.ds(pl.multiple_of(s * eighth, eighth), eighth)], wq),
        (wo_hbm.at[1, pl.ds(pl.multiple_of(s * eighth, eighth), eighth), :], wo),
        (wg_hbm.at[1, :, pl.ds(pl.multiple_of(s * wide, wide), wide)], wg),
        (wu_hbm.at[1, :, pl.ds(pl.multiple_of(s * wide, wide), wide)], wu),
        (wd_hbm.at[1, pl.ds(pl.multiple_of(s * wide, wide), wide), :], wd),
    ]
    fetches = [pltpu.make_async_copy(src, dst, w_sem.at[i]) for i, (src, dst) in enumerate(cuts)]
    for fetch in fetches:
        fetch.start()

    peers = []
    for d in range(1, 8):
        peer_b = 1 - b if d & 4 else b
        peer_a = 1 - a if d & 2 else a
        peer_s = 1 - s if d & 1 else s
        peers.append((4 * peer_b + 2 * peer_a + peer_s, {'b': peer_b, 'a': peer_a, 'stage': peer_s}))

    barrier = pltpu.get_barrier_semaphore()
    for _, where in peers:
        pl.semaphore_signal(barrier, inc=1, device_id=where, device_id_type=pl.DeviceIdType.MESH)
    pl.semaphore_wait(barrier, 7)

    def exchange(source_of, everyone, send, recv):
        copies = [
            pltpu.make_async_remote_copy(
                src_ref=source_of(peer), dst_ref=everyone.at[me], send_sem=send.at[i], recv_sem=recv.at[i],
                device_id=where, device_id_type=pl.DeviceIdType.MESH)
            for i, (peer, where) in enumerate(peers)]
        arrivals = [
            pltpu.make_async_remote_copy(
                src_ref=source_of(peer), dst_ref=everyone.at[peer], send_sem=send.at[i], recv_sem=recv.at[i],
                device_id=where, device_id_type=pl.DeviceIdType.MESH)
            for i, (peer, where) in enumerate(peers)]
        for copy in copies:
            copy.start()
        everyone[me] = source_of(me)[...]
        for arrival in arrivals:
            arrival.wait_recv()
        for copy in copies:
            copy.wait_send()

    def norm(rows, gain_ref):
        inv_rms = lax.rsqrt(jnp.mean(rows * rows, axis=-1, keepdims=True) + NORM_EPS)
        return (rows * inv_rms * gain_ref[...]).astype(jnp.bfloat16)

    row_index = lax.broadcasted_iota(jnp.int32, (n_rows, x0_ref.shape[1]), 0)
    rows = jnp.zeros((n_rows, x0_ref.shape[1]), jnp.float32)
    for c in range(n_chunk):
        last_row = x_refs[c][x_refs[c].shape[0] - 1:, :].astype(jnp.float32)
        rows = jnp.where(row_index == n_chunk * s + c, last_row, rows)
    x_src[...] = rows.astype(jnp.bfloat16)
    is_owner = a + b == 2

    def x_copy(i):
        return pltpu.make_async_remote_copy(
            src_ref=x_src, dst_ref=x_all.at[s], send_sem=x_send.at[i], recv_sem=x_recv.at[s],
            device_id=peers[i][1], device_id_type=pl.DeviceIdType.MESH)

    @pl.when(is_owner)
    def _():
        for i in range(7):
            x_copy(i).start()
        x_all[s] = x_src[...]

    for o in range(2):
        @pl.when(me != 6 + o)
        def _(o=o):
            pltpu.make_async_remote_copy(
                src_ref=x_src, dst_ref=x_all.at[o], send_sem=x_send.at[0], recv_sem=x_recv.at[o],
                device_id=peers[0][1], device_id_type=pl.DeviceIdType.MESH).wait_recv()

    @pl.when(is_owner)
    def _():
        for i in range(7):
            x_copy(i).wait_send()

    last = x_all[0].astype(jnp.float32) + x_all[1].astype(jnp.float32)
    fetches[0].wait()
    q = jnp.dot(norm(last, gain_a_ref), wq[...], preferred_element_type=jnp.float32)
    q_src[...] = q.astype(jnp.bfloat16).astype(jnp.float32)
    exchange(lambda peer: q_src, q_all, q_send, q_recv)

    kv_width = kv_heads * HEAD_DIM
    for piece in range(4):
        head_b = 1 - b if piece & 2 else b
        head_a = 1 - a if piece & 1 else a
        for h in range(kv_heads):
            head = (2 * head_b + head_a) * kv_heads + h
            low = 2 * piece * kv_width + h * HEAD_DIM
            for c in range(n_chunk):
                q_row = q_all[head, pl.ds(n_chunk * s + c, 1), :]
                q_heads = jnp.concatenate([q_row[:, g * HEAD_DIM:(g + 1) * HEAD_DIM] for g in range(group)], axis=0)
                q_heads = rotate(q_heads, cos_ref[...], sin_ref[...])
                k = kv_refs[c][:, low:low + HEAD_DIM]
                v = kv_refs[c][:, low + kv_width:low + kv_width + HEAD_DIM]
                scores = lax.dot_general(q_heads, k, (((1,), (1,)), ((), ())), preferred_element_type=jnp.float32) * HEAD_DIM ** -0.5
                top = jnp.max(scores, axis=-1, keepdims=True)
                probs = jnp.exp(scores - top)
                total = jnp.sum(probs, axis=-1, keepdims=True)
                pk_src[head, c, :, :HEAD_DIM] = jnp.dot(probs.astype(jnp.bfloat16), v, preferred_element_type=jnp.float32)
                pk_src[head, c, :, HEAD_DIM:2 * HEAD_DIM] = jnp.broadcast_to(top, (group, HEAD_DIM))
                pk_src[head, c, :, 2 * HEAD_DIM:] = jnp.broadcast_to(total, (group, HEAD_DIM))
    exchange(lambda peer: pk_src.at[peer], pk_all, pk_send, pk_recv)

    mix[...] = jnp.zeros_like(mix)
    for stage in range(2):
        for c in range(n_chunk):
            found = [pk_all[2 * i + stage, c] for i in range(4)]
            top = found[0][:, HEAD_DIM:2 * HEAD_DIM]
            for part in found[1:]:
                top = jnp.maximum(top, part[:, HEAD_DIM:2 * HEAD_DIM])
            value, total = jnp.zeros_like(top), jnp.zeros_like(top)
            for part in found:
                scale = jnp.exp(part[:, HEAD_DIM:2 * HEAD_DIM] - top)
                value += part[:, :HEAD_DIM] * scale
                total += part[:, 2 * HEAD_DIM:] * scale
            value = value / total
            for g in range(group):
                mix[n_chunk * stage + c:n_chunk * stage + c + 1, g * HEAD_DIM:(g + 1) * HEAD_DIM] = value[g:g + 1, :]

    def summed(everyone):
        total = everyone[0].astype(jnp.float32)
        for i in range(1, 8):
            total += everyone[i].astype(jnp.float32)
        return total.astype(jnp.bfloat16).astype(jnp.float32)

    fetches[1].wait()
    p_src[...] = jnp.dot(mix[...].astype(jnp.bfloat16), wo[...], preferred_element_type=jnp.float32).astype(jnp.bfloat16)
    exchange(lambda peer: p_src, p_all, p_send, p_recv)
    last = (last + summed(p_all)).astype(jnp.bfloat16).astype(jnp.float32)
    normed = norm(last, gain_m_ref)
    fetches[2].wait()
    gate = jnp.dot(normed, wg[...], preferred_element_type=jnp.float32).astype(jnp.bfloat16).astype(jnp.float32)
    fetches[3].wait()
    up = jnp.dot(normed, wu[...], preferred_element_type=jnp.float32).astype(jnp.bfloat16).astype(jnp.float32)
    act = (gate * (1.0 / (1.0 + jnp.exp(-gate))) * up).astype(jnp.bfloat16)
    fetches[4].wait()
    r_src[...] = jnp.dot(act, wd[...], preferred_element_type=jnp.float32).astype(jnp.bfloat16)
    exchange(lambda peer: r_src, r_all, r_send, r_recv)
    o_ref[...] = (last + summed(r_all)).astype(jnp.bfloat16)


def last_rows(finals, kvs, gain_a, gain_m, cos_row, sin_row, w_query, w_out, w_gate, w_up, w_down, kv_heads):
    width = finals[0].shape[1]
    eighth = w_query.shape[2] // 2
    wide = w_gate.shape[2] // 2
    group = eighth // HEAD_DIM
    n_rows = 8
    n_chunk = len(finals)
    vmem = pl.BlockSpec(memory_space=pltpu.VMEM)
    last_block = pl.BlockSpec((n_rows, width), lambda i: (finals[0].shape[0] // n_rows - 1, 0))

    def full(value):
        return pl.BlockSpec(value.shape, lambda i: (0,) * value.ndim)

    seven = pltpu.SemaphoreType.DMA((7,))
    return pl.pallas_call(
        functools.partial(tail_kernel, kv_heads),
        grid=(1,),
        in_specs=[last_block] * n_chunk + [full(kv) for kv in kvs] + [full(v) for v in (gain_a, gain_m, cos_row, sin_row)]
        + [pl.BlockSpec(memory_space=pl.ANY)] * 5,
        out_specs=pl.BlockSpec((n_rows, width), lambda i: (0, 0)),
        out_shape=jax.ShapeDtypeStruct((n_rows, width), jnp.bfloat16),
        scratch_shapes=[
            pltpu.VMEM((width, eighth), jnp.bfloat16),
            pltpu.VMEM((eighth, width), jnp.bfloat16),
            pltpu.VMEM((width, wide), jnp.bfloat16),
            pltpu.VMEM((width, wide), jnp.bfloat16),
            pltpu.VMEM((wide, width), jnp.bfloat16),
            pltpu.VMEM((n_rows, width), jnp.bfloat16),
            pltpu.VMEM((2, n_rows, width), jnp.bfloat16),
            pltpu.VMEM((n_rows, eighth), jnp.float32),
            pltpu.VMEM((8, n_rows, eighth), jnp.float32),
            pltpu.VMEM((8, n_chunk, group, 3 * HEAD_DIM), jnp.float32),
            pltpu.VMEM((8, n_chunk, group, 3 * HEAD_DIM), jnp.float32),
            pltpu.VMEM((n_rows, eighth), jnp.float32),
            pltpu.VMEM((n_rows, width), jnp.bfloat16),
            pltpu.VMEM((8, n_rows, width), jnp.bfloat16),
            pltpu.VMEM((n_rows, width), jnp.bfloat16),
            pltpu.VMEM((8, n_rows, width), jnp.bfloat16),
            pltpu.SemaphoreType.DMA((5,)),
            seven, pltpu.SemaphoreType.DMA((2,)), seven, seven, seven, seven, seven, seven, seven, seven,
        ],
        compiler_params=pltpu.CompilerParams(collective_id=0, has_side_effects=True, vmem_limit_bytes=63 * 1024 * 1024),
        cost_estimate=pl.CostEstimate(flops=9_000_000_000, bytes_accessed=60_000_000, transcendentals=0),
    )(*finals, *kvs, gain_a, gain_m, cos_row, sin_row, w_query, w_out, w_gate, w_up, w_down)


def first_cut_kernel(where_ref, near_ref, far_ref, k_ref, v_ref):
    kv_width = near_ref.shape[-1] // 2
    own_low = where_ref[0] == 0
    near, far = near_ref[0], far_ref[0]
    low, high = jnp.where(own_low, near, far), jnp.where(own_low, far, near)
    k_ref[0, 0, :, :kv_width] = low[:, :kv_width]
    k_ref[0, 0, :, kv_width:] = high[:, :kv_width]
    v_ref[0, 0, :, :kv_width] = low[:, kv_width:]
    v_ref[0, 0, :, kv_width:] = high[:, kv_width:]


def first_cut(near, far, where):
    n_chunk, seq_len, columns = near.shape
    rows = seq_len // 2
    source = pl.BlockSpec((1, rows, columns), lambda c, j, where_ref: (c, j, 0))
    target = pl.BlockSpec((1, 1, rows, columns), lambda c, j, where_ref: (0, c, j, 0))
    return pl.pallas_call(
        first_cut_kernel,
        grid_spec=pltpu.PrefetchScalarGridSpec(num_scalar_prefetch=1, grid=(n_chunk, 2), in_specs=[source] * 2, out_specs=[target] * 2),
        out_shape=[jax.ShapeDtypeStruct((2, n_chunk, seq_len, columns), jnp.bfloat16)] * 2,
        compiler_params=pltpu.CompilerParams(vmem_limit_bytes=32 * 1024 * 1024),
        cost_estimate=pl.CostEstimate(flops=1_000_000_000, bytes_accessed=19_000_000, transcendentals=0),
    )(where, near, far)


def second_cut_kernel(where_ref, near_ref, far_ref, k_in, v_in, k_ref, v_ref):
    columns = near_ref.shape[-1] // 2
    kv_width = columns // 2

    def put(source):
        mine, other = source[:, :columns], source[:, columns:]
        own_low = where_ref[0] + pl.program_id(0) - 2 * where_ref[0] * pl.program_id(0) == 0
        low, high = jnp.where(own_low, mine, other), jnp.where(own_low, other, mine)
        k_ref[0, 0, :, :kv_width] = low[:, :kv_width]
        k_ref[0, 0, :, kv_width:] = high[:, :kv_width]
        v_ref[0, 0, :, :kv_width] = low[:, kv_width:]
        v_ref[0, 0, :, kv_width:] = high[:, kv_width:]

    @pl.when(pl.program_id(0) == 0)
    def _():
        put(near_ref[0])

    @pl.when(pl.program_id(0) == 1)
    def _():
        put(far_ref[0])


def second_cut(near, far, where, k_flat, v_flat, request):
    _, rows, columns = near.shape
    block = rows // 2

    def place(i, j, half, where_ref):
        along_x = where_ref[0] + i - 2 * where_ref[0] * i
        along_y = where_ref[1] + j - 2 * where_ref[1] * j
        return 1, request, (1 - half) * (2 * along_x + along_y) + half * (4 + 2 * along_y + along_x), 0

    source = pl.BlockSpec((1, block, columns), lambda i, j, half, where_ref: (j, half, 0))
    target = pl.BlockSpec((1, 1, block, columns // 2), place)
    whole = pl.BlockSpec(memory_space=pl.ANY)
    return pl.pallas_call(
        second_cut_kernel,
        grid_spec=pltpu.PrefetchScalarGridSpec(
            num_scalar_prefetch=1, grid=(2, 2, 2), in_specs=[source] * 2 + [whole] * 2, out_specs=[target] * 2),
        out_shape=[jax.ShapeDtypeStruct(k_flat.shape, jnp.bfloat16)] * 2,
        input_output_aliases={3: 0, 4: 1},
        compiler_params=pltpu.CompilerParams(vmem_limit_bytes=32 * 1024 * 1024),
        cost_estimate=pl.CostEstimate(flops=300_000_000, bytes_accessed=5_000_000, transcendentals=0),
    )(where, near, far, k_flat, v_flat)


def solution(mesh):
    tp_axes = ('b', 'a')
    weight_cols = P(None, None, tp_axes)
    weight_rows = P(None, tp_axes, None)
    in_specs = (P('stage', 'dp', None, None), P(), weight_cols, weight_cols, weight_cols, weight_rows, P(), weight_cols, weight_cols, weight_rows)
    cache_spec = P('stage', None, ('dp', 'a'), None, 'b', None)
    out_specs = (cache_spec, cache_spec, P('stage', ('dp', 'a'), None))

    def over_x(value):
        return lax.ppermute(value, 'a', SWAP)

    def over_y(value):
        return lax.ppermute(value, 'b', SWAP)

    def across(value):
        return lax.ppermute(value, 'stage', SWAP)

    def hold(values, *after):
        return lax.optimization_barrier((values, after))[0]

    def stage_program(embeds, attn_gain, w_query, w_key, w_value, w_out, mlp_gain, w_gate, w_up, w_down):
        a, b, s = lax.axis_index('a'), lax.axis_index('b'), lax.axis_index('stage')
        n_req, seq_len, width = embeds.shape[1:]
        n_chunk = n_req // 2
        block = seq_len // 8
        kv_width = w_key.shape[2]
        kv_heads = kv_width // HEAD_DIM
        kv2 = 2 * kv_width
        half_rows = seq_len // 2
        half_width = width // 2
        cos_t, sin_t = rope_tables(seq_len)
        chip = 2 * b + a
        part = s.astype(jnp.int32).reshape(1)
        where = jnp.stack([a, b]).astype(jnp.int32)

        fours = jnp.arange(4, dtype=jnp.int32)
        order = jnp.concatenate([jnp.bitwise_xor(fours, 2 * a + b), 4 + jnp.bitwise_xor(fours, chip)]).astype(jnp.int32)

        def own_rows(value):
            return jnp.concatenate([
                lax.dynamic_slice_in_dim(value, block * (2 * a + b), block, 0),
                lax.dynamic_slice_in_dim(value, half_rows + block * chip, block, 0)], axis=0)

        def send_parts(part_sum):
            quarter = 2 * block
            return part_sum[quarter:2 * quarter], part_sum[3 * quarter:]

        def send_wide(sends):
            return over_x(sends[0]), over_y(sends[1])

        def add_wide(part_sum, got):
            quarter = 2 * block
            return add_rounded(part_sum[:quarter], got[0]), add_rounded(part_sum[2 * quarter:3 * quarter], got[1])

        def send_narrow(sums):
            return over_y(sums[0][block:]), over_x(sums[1][block:])

        def add_narrow(residual, sums, got):
            kept = jnp.concatenate([sums[0][:block], sums[1][:block]], axis=0)
            return add_rounded(residual, add_rounded(kept, jnp.concatenate(got, axis=0)))

        def gather_near(own):
            return over_y(own[:block]), over_x(own[block:])

        def join_near(own, got):
            return jnp.concatenate([own[:block], got[0]], axis=0), jnp.concatenate([own[block:], got[1]], axis=0)

        def gather_far(near):
            return over_x(near[0]), over_y(near[1])

        def join_far(near, far):
            return jnp.concatenate([near[0], far[0], near[1], far[1]], axis=0)

        def take(value):
            return lax.ppermute(value, 'stage', [(0, 1)])

        moved0 = take(embeds[0, n_chunk])

        quarter_width = width // 4

        def w_block(half, lower):
            rows = half * half_width + lower * quarter_width
            return jnp.concatenate([lax.dynamic_slice_in_dim(w[1], rows, quarter_width, 0) for w in (w_key, w_value)], axis=1)

        w_top, w_bottom = hold((w_block(s, 0), w_block(s, 1)), embeds[0, n_chunk, :8, :128])
        top_y, bottom_x = over_y(w_top), over_x(w_bottom)
        top_x, bottom_y = over_x(w_top), over_y(w_bottom)

        def project(x):
            normed = rms_norm(x, attn_gain[0])
            q = matmul(normed, w_query[0]).astype(jnp.bfloat16)
            k = matmul(normed, w_key[0]).astype(jnp.bfloat16)
            v = matmul(normed, w_value[0]).astype(jnp.bfloat16)
            return q, k, v

        def attend(q, k, v):
            mix, k_rot = attention(q, k, v, cos_t, sin_t, order)
            return matmul(mix, w_out[0]).astype(jnp.bfloat16), jnp.concatenate([k_rot, v], axis=1)

        def gate_of(normed):
            return matmul(normed, w_gate[0]).astype(jnp.bfloat16)

        def act_of(normed, gate):
            up = matmul(normed, w_up[0]).astype(jnp.bfloat16)
            return (jax.nn.silu(gate.astype(jnp.float32)) * up.astype(jnp.float32)).astype(jnp.bfloat16)

        def down_of(act):
            return matmul(act, w_down[0]).astype(jnp.bfloat16)

        def hidden_of(first, second):
            return jnp.where(s == 0, first, second)

        own_cos, own_sin = own_rows(cos_t), own_rows(sin_t)

        x0 = hidden_of(hold(embeds, moved0)[0, 0], moved0)
        qkv0 = project(x0)
        moved1 = take(hold(embeds, qkv0)[0, n_chunk + 1])
        top_d, bottom_d = over_x(hold(top_y, qkv0)), over_y(hold(bottom_x, qkv0))
        p0, kv0_0 = attend(*qkv0)
        own_x0 = own_rows(x0)
        send = send_parts(p0)
        wide0 = send_wide(send)

        moved2 = take(hold(embeds, send)[0, n_chunk + 2])
        embeds_1, moved1 = hold((embeds, moved1), send, moved1)
        x1 = hidden_of(embeds_1[0, 1], moved1)
        p1, kv0_1 = attend(*project(x1))
        own_x1 = own_rows(x1)
        send = send_parts(p1)
        wide1 = send_wide(send)

        sums0 = add_wide(p0, hold(wide0, send))
        narrow0 = send_narrow(sums0)

        embeds_2, moved2 = hold((embeds, moved2), sums0, moved2)
        x2 = hidden_of(embeds_2[0, 2], moved2)
        p2, kv0_2 = attend(*project(x2))
        own_x2 = own_rows(x2)

        sums1 = add_wide(p1, hold(wide1, p2))
        narrow1 = send_narrow(sums1)
        own1_0 = add_narrow(own_x0, sums0, hold(narrow0, sums1))
        h0 = rms_norm(own1_0, mlp_gain[0])
        near_got0 = gather_near(h0)

        own1_1 = add_narrow(own_x1, sums1, hold(narrow1, h0))
        h1 = rms_norm(own1_1, mlp_gain[0])
        near_got1 = gather_near(h1)
        near0 = join_near(h0, hold(near_got0, h1))
        far0 = gather_far(near0)
        send = hold(send_parts(p2), near0)
        wide2 = send_wide(send)
        near1 = join_near(h1, hold(near_got1, send))
        far1 = gather_far(near1)

        fetched = hold((top_x, bottom_x, top_y, bottom_y, top_d, bottom_d), near1)
        w_mine = [w_top, w_bottom] + list(fetched)
        w_other = [w_block(1 - s, 0), w_block(1 - s, 1)] + [across(piece) for piece in fetched]

        normed = join_far(near0, hold(far0, near1))
        act = act_of(normed, gate_of(normed))
        sums2 = add_wide(p2, hold(wide2, act))
        narrow2 = send_narrow(sums2)
        d0 = down_of(hold(act, sums2))
        send = send_parts(d0)
        wide0 = send_wide(send)

        normed = join_far(near1, hold(far1, send))
        gate = gate_of(normed)
        own1_2 = add_narrow(own_x2, sums2, hold(narrow2, gate))
        h2 = rms_norm(own1_2, mlp_gain[0])
        near_got2 = gather_near(h2)
        act = act_of(hold(normed, h2), gate)
        sums0 = add_wide(d0, hold(wide0, act))
        narrow0 = send_narrow(sums0)
        near2 = join_near(h2, hold(near_got2, sums0))
        far2 = gather_far(near2)
        d1 = down_of(hold(act, near2))
        send = send_parts(d1)
        wide1 = send_wide(send)

        def keys_values_of(final):
            return keys_values(final, attn_gain[1:2], w_mine, w_other, own_cos, own_sin, part)

        def to_decode(value):
            return lax.ppermute(value, ('a', 'stage'), FROM_NEAR), lax.ppermute(value, ('a', 'stage'), FROM_FAR)

        final0 = add_narrow(own1_0, sums0, hold(narrow0, send))
        kv1_0 = keys_values_of(final0)
        cut0 = to_decode(hold(jnp.stack([kv0_0, kv0_1, kv0_2]), kv1_0))

        def along_y(kv, *after):
            return over_y(hold(kv[:, 2 * kv2:], *after))

        def to_decode_rows(kv, got):
            return to_decode(jnp.stack([kv[:, :2 * kv2], got]))

        normed = join_far(near2, hold(far2, kv1_0))
        gate = gate_of(normed)
        got_0 = along_y(kv1_0, gate)
        act = act_of(normed, gate)
        sums1 = add_wide(d1, hold(wide1, act))
        narrow1 = send_narrow(sums1)
        cut1_0 = to_decode_rows(kv1_0, hold(got_0, sums1))
        d2 = down_of(hold(act, sums1))
        send = send_parts(d2)
        wide2 = send_wide(send)
        final1 = add_narrow(own1_1, sums1, hold(narrow1, send))
        kv1_1 = keys_values_of(final1)
        got_1 = along_y(kv1_1)
        k_flat, v_flat = first_cut(*hold(cut0, kv1_1), where)
        sums2 = add_wide(d2, hold(wide2, k_flat))
        narrow2 = send_narrow(sums2)
        k_flat, v_flat = second_cut(*hold(cut1_0, sums2), where, k_flat, v_flat, 0)
        final2 = add_narrow(own1_2, sums2, hold(narrow2, k_flat))
        kv1_2 = keys_values_of(final2)
        got_2 = along_y(kv1_2)
        cut1_1 = to_decode_rows(kv1_1, hold(got_1, kv1_2))
        cut1_2 = to_decode_rows(kv1_2, got_2)

        last = last_rows(
            (final0, final1, final2), (kv1_0, kv1_1, hold(kv1_2, got_2)), attn_gain[1:2], mlp_gain[1:2],
            cos_t[-1:], sin_t[-1:], w_query, w_out, w_gate, w_up, w_down, kv_heads)
        last_out = lax.dynamic_slice_in_dim(last, a * n_chunk, n_chunk, 0)
        last_out = jnp.where(s == 1, last_out, jnp.zeros_like(last_out))

        for c, cut in ((1, cut1_1), (2, cut1_2)):
            k_flat, v_flat = second_cut(*hold(cut, last), where, k_flat, v_flat, c)
        cache_shape = (1, 2, n_chunk, seq_len, 2 * kv_heads, HEAD_DIM)
        return k_flat.reshape(cache_shape), v_flat.reshape(cache_shape), last_out[None]

    return jax.shard_map(stage_program, mesh=mesh, in_specs=in_specs, out_specs=out_specs, check_vma=False)
```

```python
import functools

import jax
import jax.numpy as jnp
from jax import lax
from jax.experimental import pallas as pl
from jax.experimental.pallas import tpu as pltpu
from jax.sharding import PartitionSpec as P


HEAD_DIM = 128
ROPE_BASE = 500000.0
NORM_EPS = 1e-5
SWAP = [(0, 1), (1, 0)]
FROM_FAR = [(2, 1), (1, 3)]
FROM_NEAR = [(0, 1), (3, 3)]


def rms_norm(hidden, gain_vec):
    as_f32 = hidden.astype(jnp.float32)
    inv_rms = lax.rsqrt(jnp.mean(as_f32 * as_f32, axis=-1, keepdims=True) + NORM_EPS)
    return (as_f32 * inv_rms * gain_vec).astype(jnp.bfloat16)


def rope_tables(seq_len):
    half_dim = HEAD_DIM // 2
    inv_freq = ROPE_BASE ** (-2.0 * jnp.arange(half_dim, dtype=jnp.float32) / HEAD_DIM)
    angles = jnp.arange(seq_len, dtype=jnp.float32)[:, None] * inv_freq[None, :]
    cos_t, sin_t = jnp.cos(angles), jnp.sin(angles)
    return jnp.concatenate([cos_t, cos_t], axis=-1), jnp.concatenate([-sin_t, sin_t], axis=-1)


def matmul(left, right):
    return jnp.dot(left, right, preferred_element_type=jnp.float32)


def add_rounded(left, right):
    return (left.astype(jnp.float32) + right.astype(jnp.float32)).astype(jnp.bfloat16)


def rotate(as_f32, cos_rows, sin_rows):
    return (as_f32 * cos_rows + pltpu.roll(as_f32, HEAD_DIM // 2, 1) * sin_rows).astype(jnp.bfloat16)


def attention_kernel(q_block, group, _, q_ref, k_ref, v_ref, cos_ref, sin_ref, o_ref, kr_ref):
    step = pl.program_id(1)
    seq_len = k_ref.shape[0]

    @pl.when(step == 0)
    def _():
        kr_ref[...] = rotate(k_ref[...].astype(jnp.float32), cos_ref[...], sin_ref[...])

    for i in range(seq_len // q_block):
        @pl.when(step == i)
        def _(i=i):
            keys = min(seq_len, -(-(i + 1) * q_block // 128) * 128)
            rows = pl.ds(i * q_block, q_block)
            cos_rows, sin_rows = cos_ref[rows, :], sin_ref[rows, :]
            q = jnp.concatenate([
                rotate(q_ref[:, g * HEAD_DIM:(g + 1) * HEAD_DIM].astype(jnp.float32), cos_rows, sin_rows)
                for g in range(group)], axis=0)
            row = lax.rem(lax.broadcasted_iota(jnp.int32, (group * q_block, keys), 0), q_block) + i * q_block
            col = lax.broadcasted_iota(jnp.int32, (group * q_block, keys), 1)
            scores = lax.dot_general(q, kr_ref[:keys, :], (((1,), (1,)), ((), ())), preferred_element_type=jnp.float32)
            scores = jnp.where(row >= col, scores * HEAD_DIM ** -0.5, -1e30)
            probs = jnp.exp(scores - jnp.max(scores, axis=-1, keepdims=True))
            probs = probs * (1.0 / jnp.sum(probs, axis=-1, keepdims=True))
            mix = jnp.dot(probs.astype(jnp.bfloat16), v_ref[:keys, :], preferred_element_type=jnp.float32).astype(jnp.bfloat16)
            for g in range(group):
                o_ref[:, g * HEAD_DIM:(g + 1) * HEAD_DIM] = mix[g * q_block:(g + 1) * q_block]


def attention(q, k, v, cos_t, sin_t, order):
    seq_len, kv_width = k.shape
    q_block = seq_len // 8
    group = q.shape[1] // kv_width
    wide = group * HEAD_DIM
    return pl.pallas_call(
        functools.partial(attention_kernel, q_block, group),
        grid_spec=pltpu.PrefetchScalarGridSpec(
            num_scalar_prefetch=1,
            grid=(kv_width // HEAD_DIM, 8),
            in_specs=[
                pl.BlockSpec((q_block, wide), lambda h, i, order_ref: (i, h)),
                pl.BlockSpec((seq_len, HEAD_DIM), lambda h, i, order_ref: (0, h)),
                pl.BlockSpec((seq_len, HEAD_DIM), lambda h, i, order_ref: (0, h)),
                pl.BlockSpec((seq_len, HEAD_DIM), lambda h, i, order_ref: (0, 0)),
                pl.BlockSpec((seq_len, HEAD_DIM), lambda h, i, order_ref: (0, 0)),
            ],
            out_specs=[
                pl.BlockSpec((q_block, wide), lambda h, i, order_ref: (order_ref[i], h)),
                pl.BlockSpec((seq_len, HEAD_DIM), lambda h, i, order_ref: (0, h)),
            ],
        ),
        out_shape=[jax.ShapeDtypeStruct(q.shape, jnp.bfloat16), jax.ShapeDtypeStruct(k.shape, jnp.bfloat16)],
        compiler_params=pltpu.CompilerParams(vmem_limit_bytes=32 * 1024 * 1024),
        cost_estimate=pl.CostEstimate(flops=9_000_000_000, bytes_accessed=5_000_000, transcendentals=4_000_000),
    )(order, q, k, v, cos_t, sin_t)


def kv_kernel(part_ref, x_ref, gain_ref, cos_ref, sin_ref, *refs):
    mine, other, o_ref, normed = refs[:8], refs[8:16], refs[16], refs[17]
    depth, columns = mine[0].shape
    half = 2 * depth
    as_f32 = x_ref[...].astype(jnp.float32)
    inv_rms = lax.rsqrt(jnp.mean(as_f32 * as_f32, axis=-1, keepdims=True) + NORM_EPS)
    whole = (as_f32 * inv_rms * gain_ref[...]).astype(jnp.bfloat16)
    normed[0] = whole[:, :half]
    normed[1] = whole[:, half:]
    part = part_ref[0]
    for piece in range(4):
        product = jnp.dot(normed[part, :, :depth], mine[2 * piece][...], preferred_element_type=jnp.float32)
        product += jnp.dot(normed[part, :, depth:], mine[2 * piece + 1][...], preferred_element_type=jnp.float32)
        product += jnp.dot(normed[1 - part, :, :depth], other[2 * piece][...], preferred_element_type=jnp.float32)
        product += jnp.dot(normed[1 - part, :, depth:], other[2 * piece + 1][...], preferred_element_type=jnp.float32)
        rounded = product.astype(jnp.bfloat16)
        base = piece * columns
        for h in range(columns // 2 // HEAD_DIM):
            cols = slice(h * HEAD_DIM, (h + 1) * HEAD_DIM)
            o_ref[:, base + h * HEAD_DIM:base + (h + 1) * HEAD_DIM] = rotate(rounded[:, cols].astype(jnp.float32), cos_ref[...], sin_ref[...])
        o_ref[:, base + columns // 2:base + columns] = rounded[:, columns // 2:]


def keys_values(x, gain, mine, other, cos_rows, sin_rows, part):
    rows, _ = x.shape
    depth, columns = mine[0].shape
    vmem = pl.BlockSpec(memory_space=pltpu.VMEM)
    return pl.pallas_call(
        kv_kernel,
        in_specs=[pl.BlockSpec(memory_space=pltpu.SMEM)] + [vmem] * 20,
        out_specs=vmem,
        out_shape=jax.ShapeDtypeStruct((rows, 4 * columns), jnp.bfloat16),
        scratch_shapes=[pltpu.VMEM((2, rows, 2 * depth), jnp.bfloat16)],
        compiler_params=pltpu.CompilerParams(vmem_limit_bytes=40 * 1024 * 1024),
        cost_estimate=pl.CostEstimate(flops=32 * rows * depth * columns, bytes_accessed=32 * depth * columns, transcendentals=0),
    )(part, x, gain, cos_rows, sin_rows, *mine, *other)


def tail_kernel(kv_heads, x0_ref, x1_ref, x2_ref, kv0_ref, kv1_ref, kv2_ref, gain_a_ref, gain_m_ref, cos_ref, sin_ref,
                wq_hbm, wo_hbm, wg_hbm, wu_hbm, wd_hbm, o_ref,
                wq, wo, wg, wu, wd, x_src, x_all, q_src, q_all, pk_src, pk_all, mix, p_src, p_all, r_src, r_all,
                w_sem, x_send, x_recv, q_send, q_recv, pk_send, pk_recv, p_send, p_recv, r_send, r_recv):
    a, b, s = lax.axis_index('a'), lax.axis_index('b'), lax.axis_index('stage')
    me = 4 * b + 2 * a + s
    x_refs, kv_refs = (x0_ref, x1_ref, x2_ref), (kv0_ref, kv1_ref, kv2_ref)
    n_chunk = len(x_refs)
    n_rows = o_ref.shape[0]
    group = wq.shape[1] // HEAD_DIM
    eighth, wide = wq.shape[1], wg.shape[1]

    cuts = [
        (wq_hbm.at[1, :, pl.ds(pl.multiple_of(s * eighth, eighth), eighth)], wq),
        (wo_hbm.at[1, pl.ds(pl.multiple_of(s * eighth, eighth), eighth), :], wo),
        (wg_hbm.at[1, :, pl.ds(pl.multiple_of(s * wide, wide), wide)], wg),
        (wu_hbm.at[1, :, pl.ds(pl.multiple_of(s * wide, wide), wide)], wu),
        (wd_hbm.at[1, pl.ds(pl.multiple_of(s * wide, wide), wide), :], wd),
    ]
    fetches = [pltpu.make_async_copy(src, dst, w_sem.at[i]) for i, (src, dst) in enumerate(cuts)]
    for fetch in fetches:
        fetch.start()

    peers = []
    for d in range(1, 8):
        peer_b = 1 - b if d & 4 else b
        peer_a = 1 - a if d & 2 else a
        peer_s = 1 - s if d & 1 else s
        peers.append((4 * peer_b + 2 * peer_a + peer_s, {'b': peer_b, 'a': peer_a, 'stage': peer_s}))

    barrier = pltpu.get_barrier_semaphore()
    for _, where in peers:
        pl.semaphore_signal(barrier, inc=1, device_id=where, device_id_type=pl.DeviceIdType.MESH)
    pl.semaphore_wait(barrier, 7)

    def exchange(source_of, everyone, send, recv):
        copies = [
            pltpu.make_async_remote_copy(
                src_ref=source_of(peer), dst_ref=everyone.at[me], send_sem=send.at[i], recv_sem=recv.at[i],
                device_id=where, device_id_type=pl.DeviceIdType.MESH)
            for i, (peer, where) in enumerate(peers)]
        arrivals = [
            pltpu.make_async_remote_copy(
                src_ref=source_of(peer), dst_ref=everyone.at[peer], send_sem=send.at[i], recv_sem=recv.at[i],
                device_id=where, device_id_type=pl.DeviceIdType.MESH)
            for i, (peer, where) in enumerate(peers)]
        for copy in copies:
            copy.start()
        everyone[me] = source_of(me)[...]
        for arrival in arrivals:
            arrival.wait_recv()
        for copy in copies:
            copy.wait_send()

    def norm(rows, gain_ref):
        inv_rms = lax.rsqrt(jnp.mean(rows * rows, axis=-1, keepdims=True) + NORM_EPS)
        return (rows * inv_rms * gain_ref[...]).astype(jnp.bfloat16)

    row_index = lax.broadcasted_iota(jnp.int32, (n_rows, x0_ref.shape[1]), 0)
    rows = jnp.zeros((n_rows, x0_ref.shape[1]), jnp.float32)
    for c in range(n_chunk):
        last_row = x_refs[c][x_refs[c].shape[0] - 1:, :].astype(jnp.float32)
        rows = jnp.where(row_index == n_chunk * s + c, last_row, rows)
    x_src[...] = rows.astype(jnp.bfloat16)
    is_owner = a + b == 2

    def x_copy(i):
        return pltpu.make_async_remote_copy(
            src_ref=x_src, dst_ref=x_all.at[s], send_sem=x_send.at[i], recv_sem=x_recv.at[s],
            device_id=peers[i][1], device_id_type=pl.DeviceIdType.MESH)

    @pl.when(is_owner)
    def _():
        for i in range(7):
            x_copy(i).start()
        x_all[s] = x_src[...]

    for o in range(2):
        @pl.when(me != 6 + o)
        def _(o=o):
            pltpu.make_async_remote_copy(
                src_ref=x_src, dst_ref=x_all.at[o], send_sem=x_send.at[0], recv_sem=x_recv.at[o],
                device_id=peers[0][1], device_id_type=pl.DeviceIdType.MESH).wait_recv()

    @pl.when(is_owner)
    def _():
        for i in range(7):
            x_copy(i).wait_send()

    last = x_all[0].astype(jnp.float32) + x_all[1].astype(jnp.float32)
    fetches[0].wait()
    q = jnp.dot(norm(last, gain_a_ref), wq[...], preferred_element_type=jnp.float32)
    q_src[...] = q.astype(jnp.bfloat16).astype(jnp.float32)
    exchange(lambda peer: q_src, q_all, q_send, q_recv)

    kv_width = kv_heads * HEAD_DIM
    for piece in range(4):
        head_b = 1 - b if piece & 2 else b
        head_a = 1 - a if piece & 1 else a
        for h in range(kv_heads):
            head = (2 * head_b + head_a) * kv_heads + h
            low = 2 * piece * kv_width + h * HEAD_DIM
            for c in range(n_chunk):
                q_row = q_all[head, pl.ds(n_chunk * s + c, 1), :]
                q_heads = jnp.concatenate([q_row[:, g * HEAD_DIM:(g + 1) * HEAD_DIM] for g in range(group)], axis=0)
                q_heads = rotate(q_heads, cos_ref[...], sin_ref[...])
                k = kv_refs[c][:, low:low + HEAD_DIM]
                v = kv_refs[c][:, low + kv_width:low + kv_width + HEAD_DIM]
                scores = lax.dot_general(q_heads, k, (((1,), (1,)), ((), ())), preferred_element_type=jnp.float32) * HEAD_DIM ** -0.5
                top = jnp.max(scores, axis=-1, keepdims=True)
                probs = jnp.exp(scores - top)
                total = jnp.sum(probs, axis=-1, keepdims=True)
                pk_src[head, c, :, :HEAD_DIM] = jnp.dot(probs.astype(jnp.bfloat16), v, preferred_element_type=jnp.float32)
                pk_src[head, c, :, HEAD_DIM:2 * HEAD_DIM] = jnp.broadcast_to(top, (group, HEAD_DIM))
                pk_src[head, c, :, 2 * HEAD_DIM:] = jnp.broadcast_to(total, (group, HEAD_DIM))
    exchange(lambda peer: pk_src.at[peer], pk_all, pk_send, pk_recv)

    mix[...] = jnp.zeros_like(mix)
    for stage in range(2):
        for c in range(n_chunk):
            found = [pk_all[2 * i + stage, c] for i in range(4)]
            top = found[0][:, HEAD_DIM:2 * HEAD_DIM]
            for part in found[1:]:
                top = jnp.maximum(top, part[:, HEAD_DIM:2 * HEAD_DIM])
            value, total = jnp.zeros_like(top), jnp.zeros_like(top)
            for part in found:
                scale = jnp.exp(part[:, HEAD_DIM:2 * HEAD_DIM] - top)
                value += part[:, :HEAD_DIM] * scale
                total += part[:, 2 * HEAD_DIM:] * scale
            value = value / total
            for g in range(group):
                mix[n_chunk * stage + c:n_chunk * stage + c + 1, g * HEAD_DIM:(g + 1) * HEAD_DIM] = value[g:g + 1, :]

    def summed(everyone):
        total = everyone[0].astype(jnp.float32)
        for i in range(1, 8):
            total += everyone[i].astype(jnp.float32)
        return total.astype(jnp.bfloat16).astype(jnp.float32)

    fetches[1].wait()
    p_src[...] = jnp.dot(mix[...].astype(jnp.bfloat16), wo[...], preferred_element_type=jnp.float32).astype(jnp.bfloat16)
    exchange(lambda peer: p_src, p_all, p_send, p_recv)
    last = (last + summed(p_all)).astype(jnp.bfloat16).astype(jnp.float32)
    normed = norm(last, gain_m_ref)
    fetches[2].wait()
    gate = jnp.dot(normed, wg[...], preferred_element_type=jnp.float32).astype(jnp.bfloat16).astype(jnp.float32)
    fetches[3].wait()
    up = jnp.dot(normed, wu[...], preferred_element_type=jnp.float32).astype(jnp.bfloat16).astype(jnp.float32)
    act = (gate * (1.0 / (1.0 + jnp.exp(-gate))) * up).astype(jnp.bfloat16)
    fetches[4].wait()
    r_src[...] = jnp.dot(act, wd[...], preferred_element_type=jnp.float32).astype(jnp.bfloat16)
    exchange(lambda peer: r_src, r_all, r_send, r_recv)
    o_ref[...] = (last + summed(r_all)).astype(jnp.bfloat16)


def last_rows(finals, kvs, gain_a, gain_m, cos_row, sin_row, w_query, w_out, w_gate, w_up, w_down, kv_heads):
    width = finals[0].shape[1]
    eighth = w_query.shape[2] // 2
    wide = w_gate.shape[2] // 2
    group = eighth // HEAD_DIM
    n_rows = 8
    n_chunk = len(finals)
    vmem = pl.BlockSpec(memory_space=pltpu.VMEM)
    last_block = pl.BlockSpec((n_rows, width), lambda i: (finals[0].shape[0] // n_rows - 1, 0))

    def full(value):
        return pl.BlockSpec(value.shape, lambda i: (0,) * value.ndim)

    seven = pltpu.SemaphoreType.DMA((7,))
    return pl.pallas_call(
        functools.partial(tail_kernel, kv_heads),
        grid=(1,),
        in_specs=[last_block] * n_chunk + [full(kv) for kv in kvs] + [full(v) for v in (gain_a, gain_m, cos_row, sin_row)]
        + [pl.BlockSpec(memory_space=pl.ANY)] * 5,
        out_specs=pl.BlockSpec((n_rows, width), lambda i: (0, 0)),
        out_shape=jax.ShapeDtypeStruct((n_rows, width), jnp.bfloat16),
        scratch_shapes=[
            pltpu.VMEM((width, eighth), jnp.bfloat16),
            pltpu.VMEM((eighth, width), jnp.bfloat16),
            pltpu.VMEM((width, wide), jnp.bfloat16),
            pltpu.VMEM((width, wide), jnp.bfloat16),
            pltpu.VMEM((wide, width), jnp.bfloat16),
            pltpu.VMEM((n_rows, width), jnp.bfloat16),
            pltpu.VMEM((2, n_rows, width), jnp.bfloat16),
            pltpu.VMEM((n_rows, eighth), jnp.float32),
            pltpu.VMEM((8, n_rows, eighth), jnp.float32),
            pltpu.VMEM((8, n_chunk, group, 3 * HEAD_DIM), jnp.float32),
            pltpu.VMEM((8, n_chunk, group, 3 * HEAD_DIM), jnp.float32),
            pltpu.VMEM((n_rows, eighth), jnp.float32),
            pltpu.VMEM((n_rows, width), jnp.bfloat16),
            pltpu.VMEM((8, n_rows, width), jnp.bfloat16),
            pltpu.VMEM((n_rows, width), jnp.bfloat16),
            pltpu.VMEM((8, n_rows, width), jnp.bfloat16),
            pltpu.SemaphoreType.DMA((5,)),
            seven, pltpu.SemaphoreType.DMA((2,)), seven, seven, seven, seven, seven, seven, seven, seven,
        ],
        compiler_params=pltpu.CompilerParams(collective_id=0, has_side_effects=True, vmem_limit_bytes=63 * 1024 * 1024),
        cost_estimate=pl.CostEstimate(flops=9_000_000_000, bytes_accessed=60_000_000, transcendentals=0),
    )(*finals, *kvs, gain_a, gain_m, cos_row, sin_row, w_query, w_out, w_gate, w_up, w_down)


def write_heads(k_ref, v_ref, low, high):
    rows, kv2 = low.shape
    for ref, start in ((k_ref, 0), (v_ref, kv2 // 2)):
        heads = jnp.concatenate([low[:, start:start + kv2 // 2], high[:, start:start + kv2 // 2]], axis=1)
        ref[0, 0, 0] = heads.reshape(rows, kv2 // HEAD_DIM, HEAD_DIM)


def first_cut_kernel(where_ref, near_ref, far_ref, k_ref, v_ref):
    own_low = where_ref[0] == 0
    near, far = near_ref[0], far_ref[0]
    write_heads(k_ref, v_ref, jnp.where(own_low, near, far), jnp.where(own_low, far, near))


def first_cut(near, far, where):
    n_chunk, seq_len, columns = near.shape
    rows = seq_len // 2
    heads = columns // HEAD_DIM
    source = pl.BlockSpec((1, rows, columns), lambda c, j, where_ref: (c, j, 0))
    target = pl.BlockSpec((1, 1, 1, rows, heads, HEAD_DIM), lambda c, j, where_ref: (0, 0, c, j, 0, 0))
    return pl.pallas_call(
        first_cut_kernel,
        grid_spec=pltpu.PrefetchScalarGridSpec(num_scalar_prefetch=1, grid=(n_chunk, 2), in_specs=[source] * 2, out_specs=[target] * 2),
        out_shape=[jax.ShapeDtypeStruct((1, 2, n_chunk, seq_len, heads, HEAD_DIM), jnp.bfloat16)] * 2,
        compiler_params=pltpu.CompilerParams(vmem_limit_bytes=32 * 1024 * 1024),
        cost_estimate=pl.CostEstimate(flops=1_000_000_000, bytes_accessed=19_000_000, transcendentals=0),
    )(where, near, far)


def second_cut_kernel(where_ref, near_ref, far_ref, k_in, v_in, k_ref, v_ref):
    columns = near_ref.shape[-1] // 2

    def put(source):
        mine, other = source[:, :columns], source[:, columns:]
        own_low = where_ref[0] + pl.program_id(0) - 2 * where_ref[0] * pl.program_id(0) == 0
        write_heads(k_ref, v_ref, jnp.where(own_low, mine, other), jnp.where(own_low, other, mine))

    @pl.when(pl.program_id(0) == 0)
    def _():
        put(near_ref[0])

    @pl.when(pl.program_id(0) == 1)
    def _():
        put(far_ref[0])


def second_cut(near, far, where, k_cache, v_cache, request):
    _, rows, columns = near.shape
    block = rows // 2
    heads = columns // 2 // HEAD_DIM

    def place(i, j, half, where_ref):
        along_x = where_ref[0] + i - 2 * where_ref[0] * i
        along_y = where_ref[1] + j - 2 * where_ref[1] * j
        return 0, 1, request, (1 - half) * (2 * along_x + along_y) + half * (4 + 2 * along_y + along_x), 0, 0

    source = pl.BlockSpec((1, block, columns), lambda i, j, half, where_ref: (j, half, 0))
    target = pl.BlockSpec((1, 1, 1, block, heads, HEAD_DIM), place)
    whole = pl.BlockSpec(memory_space=pl.ANY)
    return pl.pallas_call(
        second_cut_kernel,
        grid_spec=pltpu.PrefetchScalarGridSpec(
            num_scalar_prefetch=1, grid=(2, 2, 2), in_specs=[source] * 2 + [whole] * 2, out_specs=[target] * 2),
        out_shape=[jax.ShapeDtypeStruct(k_cache.shape, jnp.bfloat16)] * 2,
        input_output_aliases={3: 0, 4: 1},
        compiler_params=pltpu.CompilerParams(vmem_limit_bytes=32 * 1024 * 1024),
        cost_estimate=pl.CostEstimate(flops=300_000_000, bytes_accessed=5_000_000, transcendentals=0),
    )(where, near, far, k_cache, v_cache)


def solution(mesh):
    tp_axes = ('b', 'a')
    weight_cols = P(None, None, tp_axes)
    weight_rows = P(None, tp_axes, None)
    in_specs = (P('stage', 'dp', None, None), P(), weight_cols, weight_cols, weight_cols, weight_rows, P(), weight_cols, weight_cols, weight_rows)
    cache_spec = P('stage', None, ('dp', 'a'), None, 'b', None)
    out_specs = (cache_spec, cache_spec, P('stage', ('dp', 'a'), None))

    def over_x(value):
        return lax.ppermute(value, 'a', SWAP)

    def over_y(value):
        return lax.ppermute(value, 'b', SWAP)

    def across(value):
        return lax.ppermute(value, 'stage', SWAP)

    def hold(values, *after):
        return lax.optimization_barrier((values, after))[0]

    def stage_program(embeds, attn_gain, w_query, w_key, w_value, w_out, mlp_gain, w_gate, w_up, w_down):
        a, b, s = lax.axis_index('a'), lax.axis_index('b'), lax.axis_index('stage')
        n_req, seq_len, width = embeds.shape[1:]
        n_chunk = n_req // 2
        block = seq_len // 8
        kv_width = w_key.shape[2]
        kv_heads = kv_width // HEAD_DIM
        kv2 = 2 * kv_width
        half_rows = seq_len // 2
        half_width = width // 2
        cos_t, sin_t = rope_tables(seq_len)
        chip = 2 * b + a
        part = s.astype(jnp.int32).reshape(1)
        where = jnp.stack([a, b]).astype(jnp.int32)

        fours = jnp.arange(4, dtype=jnp.int32)
        order = jnp.concatenate([jnp.bitwise_xor(fours, 2 * a + b), 4 + jnp.bitwise_xor(fours, chip)]).astype(jnp.int32)

        def own_rows(value):
            return jnp.concatenate([
                lax.dynamic_slice_in_dim(value, block * (2 * a + b), block, 0),
                lax.dynamic_slice_in_dim(value, half_rows + block * chip, block, 0)], axis=0)

        def send_parts(part_sum):
            quarter = 2 * block
            return part_sum[quarter:2 * quarter], part_sum[3 * quarter:]

        def send_wide(sends):
            return over_x(sends[0]), over_y(sends[1])

        def add_wide(part_sum, got):
            quarter = 2 * block
            return add_rounded(part_sum[:quarter], got[0]), add_rounded(part_sum[2 * quarter:3 * quarter], got[1])

        def send_narrow(sums):
            return over_y(sums[0][block:]), over_x(sums[1][block:])

        def add_narrow(residual, sums, got):
            kept = jnp.concatenate([sums[0][:block], sums[1][:block]], axis=0)
            return add_rounded(residual, add_rounded(kept, jnp.concatenate(got, axis=0)))

        def gather_near(own):
            return over_y(own[:block]), over_x(own[block:])

        def join_near(own, got):
            return jnp.concatenate([own[:block], got[0]], axis=0), jnp.concatenate([own[block:], got[1]], axis=0)

        def gather_far(near):
            return over_x(near[0]), over_y(near[1])

        def join_far(near, far):
            return jnp.concatenate([near[0], far[0], near[1], far[1]], axis=0)

        def take(value):
            return lax.ppermute(value, 'stage', [(0, 1)])

        moved0 = take(embeds[0, n_chunk])

        quarter_width = width // 4

        def w_block(half, lower):
            rows = half * half_width + lower * quarter_width
            return jnp.concatenate([lax.dynamic_slice_in_dim(w[1], rows, quarter_width, 0) for w in (w_key, w_value)], axis=1)

        w_top, w_bottom = hold((w_block(s, 0), w_block(s, 1)), embeds[0, n_chunk, :8, :128])
        top_y, bottom_x = over_y(w_top), over_x(w_bottom)
        top_x, bottom_y = over_x(w_top), over_y(w_bottom)

        def project(x):
            normed = rms_norm(x, attn_gain[0])
            q = matmul(normed, w_query[0]).astype(jnp.bfloat16)
            k = matmul(normed, w_key[0]).astype(jnp.bfloat16)
            v = matmul(normed, w_value[0]).astype(jnp.bfloat16)
            return q, k, v

        def attend(qkv):
            mix, k_rot = attention(*qkv, cos_t, sin_t, order)
            return mix, jnp.concatenate([k_rot, qkv[2]], axis=1)

        def out_of(mix):
            return matmul(mix, w_out[0]).astype(jnp.bfloat16)

        def gate_of(normed):
            return matmul(normed, w_gate[0]).astype(jnp.bfloat16)

        def act_of(normed, gate):
            up = matmul(normed, w_up[0]).astype(jnp.bfloat16)
            return (jax.nn.silu(gate.astype(jnp.float32)) * up.astype(jnp.float32)).astype(jnp.bfloat16)

        def down_of(act):
            return matmul(act, w_down[0]).astype(jnp.bfloat16)

        def hidden_of(first, second):
            return jnp.where(s == 0, first, second)

        own_cos, own_sin = own_rows(cos_t), own_rows(sin_t)

        x0 = hidden_of(hold(embeds, moved0)[0, 0], moved0)
        qkv0 = project(x0)
        moved1 = take(hold(embeds, qkv0)[0, n_chunk + 1])
        top_d, bottom_d = over_x(hold(top_y, qkv0)), over_y(hold(bottom_x, qkv0))
        mix0, kv0_0 = attend(qkv0)
        p0 = out_of(mix0)
        own_x0 = own_rows(x0)
        send = send_parts(p0)
        wide0 = send_wide(send)

        moved2 = take(hold(embeds, send)[0, n_chunk + 2])
        embeds_1, moved1 = hold((embeds, moved1), send, moved1)
        x1 = hidden_of(embeds_1[0, 1], moved1)
        qkv1 = project(x1)
        sums0 = add_wide(p0, hold(wide0, qkv1))
        narrow0 = send_narrow(sums0)
        mix1, kv0_1 = attend(hold(qkv1, sums0))
        own1_0 = add_narrow(own_x0, sums0, hold(narrow0, mix1))
        h0 = rms_norm(own1_0, mlp_gain[0])
        near_got0 = gather_near(h0)
        p1 = out_of(hold(mix1, h0))
        own_x1 = own_rows(x1)
        send = send_parts(p1)
        wide1 = send_wide(send)
        near0 = join_near(h0, hold(near_got0, send))
        far0 = gather_far(near0)

        embeds_2, moved2 = hold((embeds, moved2), near0, moved2)
        x2 = hidden_of(embeds_2[0, 2], moved2)
        qkv2 = project(x2)
        mix2, kv0_2 = attend(qkv2)
        sums1 = add_wide(p1, hold(wide1, mix2))
        narrow1 = send_narrow(sums1)
        p2 = out_of(hold(mix2, sums1))
        own_x2 = own_rows(x2)
        send = send_parts(p2)
        wide2 = send_wide(send)

        normed = join_far(near0, hold(far0, send))
        gate = gate_of(normed)
        own1_1 = add_narrow(own_x1, sums1, hold(narrow1, gate))
        h1 = rms_norm(own1_1, mlp_gain[0])
        near_got1 = gather_near(h1)
        act = act_of(hold(normed, h1), gate)
        near1 = join_near(h1, hold(near_got1, act))
        far1 = gather_far(near1)
        sums2 = add_wide(p2, hold(wide2, near1))
        narrow2 = send_narrow(sums2)
        d0 = down_of(hold(act, sums2))
        send = send_parts(d0)
        wide0 = send_wide(send)

        fetched = hold((top_x, bottom_x, top_y, bottom_y, top_d, bottom_d), send)
        w_mine = [w_top, w_bottom] + list(fetched)
        w_other = [w_block(1 - s, 0), w_block(1 - s, 1)] + [across(piece) for piece in fetched]

        normed = join_far(near1, hold(far1, send))
        gate = gate_of(normed)
        own1_2 = add_narrow(own_x2, sums2, hold(narrow2, gate))
        h2 = rms_norm(own1_2, mlp_gain[0])
        near_got2 = gather_near(h2)
        act = act_of(hold(normed, h2), gate)
        near2 = join_near(h2, hold(near_got2, act))
        far2 = gather_far(near2)
        sums0 = add_wide(d0, hold(wide0, near2))
        narrow0 = send_narrow(sums0)
        d1 = down_of(hold(act, sums0))
        send = send_parts(d1)
        wide1 = send_wide(send)

        def keys_values_of(final):
            return keys_values(final, attn_gain[1:2], w_mine, w_other, own_cos, own_sin, part)

        def to_decode(value):
            return lax.ppermute(value, ('a', 'stage'), FROM_NEAR), lax.ppermute(value, ('a', 'stage'), FROM_FAR)

        def along_y(kv, *after):
            return over_y(hold(kv[:, 2 * kv2:], *after))

        def to_decode_rows(kv, got):
            return to_decode(jnp.stack([kv[:, :2 * kv2], got]))

        normed = join_far(near2, hold(far2, send))
        gate = gate_of(normed)
        final0 = add_narrow(own1_0, sums0, hold(narrow0, gate))
        kv1_0 = keys_values_of(final0)
        got_0 = along_y(kv1_0)
        cut0 = to_decode(hold(jnp.stack([kv0_0, kv0_1, kv0_2]), kv1_0))
        act = act_of(hold(normed, kv1_0), gate)
        sums1 = add_wide(d1, hold(wide1, act))
        narrow1 = send_narrow(sums1)
        cut1_0 = to_decode_rows(kv1_0, hold(got_0, sums1))
        d2 = down_of(hold(act, sums1))
        send = send_parts(d2)
        wide2 = send_wide(send)
        final1 = add_narrow(own1_1, sums1, hold(narrow1, send))
        kv1_1 = keys_values_of(final1)
        got_1 = along_y(kv1_1)
        k_cache, v_cache = first_cut(*hold(cut0, kv1_1), where)
        sums2 = add_wide(d2, hold(wide2, k_cache))
        narrow2 = send_narrow(sums2)
        k_cache, v_cache = second_cut(*hold(cut1_0, sums2), where, k_cache, v_cache, 0)
        final2 = add_narrow(own1_2, sums2, hold(narrow2, k_cache))
        kv1_2 = keys_values_of(final2)
        got_2 = along_y(kv1_2)
        cut1_1 = to_decode_rows(kv1_1, hold(got_1, kv1_2))
        cut1_2 = to_decode_rows(kv1_2, got_2)

        last = last_rows(
            (final0, final1, final2), (kv1_0, kv1_1, hold(kv1_2, got_2)), attn_gain[1:2], mlp_gain[1:2],
            cos_t[-1:], sin_t[-1:], w_query, w_out, w_gate, w_up, w_down, kv_heads)
        last_out = lax.dynamic_slice_in_dim(last, a * n_chunk, n_chunk, 0)
        last_out = jnp.where(s == 1, last_out, jnp.zeros_like(last_out))

        for c, cut in ((1, cut1_1), (2, cut1_2)):
            k_cache, v_cache = second_cut(*hold(cut, last), where, k_cache, v_cache, c)
        return k_cache, v_cache, last_out[None]

    return jax.shard_map(stage_program, mesh=mesh, in_specs=in_specs, out_specs=out_specs, check_vma=False)
```

```python
import functools

import jax
import jax.numpy as jnp
from jax import lax
from jax.experimental import pallas as pl
from jax.experimental.pallas import tpu as pltpu
from jax.sharding import PartitionSpec as P


HEAD_DIM = 128
ROPE_BASE = 500000.0
NORM_EPS = 1e-5
MIB = 1 << 20
SWAP = [(0, 1), (1, 0)]
FROM_FAR = [(2, 1), (1, 3)]
FROM_NEAR = [(0, 1), (3, 3)]


def rms_norm(hidden, gain_vec):
    as_f32 = hidden.astype(jnp.float32)
    inv_rms = lax.rsqrt(jnp.mean(as_f32 * as_f32, axis=-1, keepdims=True) + NORM_EPS)
    return (as_f32 * inv_rms * gain_vec).astype(jnp.bfloat16)


def rope_tables(seq_len):
    half_dim = HEAD_DIM // 2
    inv_freq = ROPE_BASE ** (-2.0 * jnp.arange(half_dim, dtype=jnp.float32) / HEAD_DIM)
    angles = jnp.arange(seq_len, dtype=jnp.float32)[:, None] * inv_freq[None, :]
    cos_t, sin_t = jnp.cos(angles), jnp.sin(angles)
    return jnp.concatenate([cos_t, cos_t], axis=-1), jnp.concatenate([-sin_t, sin_t], axis=-1)


def matmul(left, right):
    return jnp.dot(left, right, preferred_element_type=jnp.float32)


def params(mebibytes, **extra):
    return pltpu.CompilerParams(vmem_limit_bytes=mebibytes * MIB, **extra)


def cost(flops, bytes_accessed):
    return pl.CostEstimate(flops=flops, bytes_accessed=bytes_accessed, transcendentals=0)


def normalised(as_f32, gain_ref):
    inv_rms = lax.rsqrt(jnp.mean(as_f32 * as_f32, axis=-1, keepdims=True) + NORM_EPS)
    return (as_f32 * inv_rms * gain_ref[:]).astype(jnp.bfloat16)


def gated(gate, up):
    return (gate * (1.0 / (1.0 + jnp.exp(-gate))) * up).astype(jnp.bfloat16)


def add_rounded(left, right):
    return (left.astype(jnp.float32) + right.astype(jnp.float32)).astype(jnp.bfloat16)


def rotate(as_f32, cos_rows, sin_rows):
    return (as_f32 * cos_rows + pltpu.roll(as_f32, HEAD_DIM // 2, 1) * sin_rows).astype(jnp.bfloat16)


def attention_kernel(q_block, group, _, q_ref, k_ref, v_ref, cos_ref, sin_ref, o_ref, kr_ref):
    step = pl.program_id(1)
    seq_len = k_ref.shape[0]

    @pl.when(step == 0)
    def _():
        kr_ref[:] = rotate(k_ref[:].astype(jnp.float32), cos_ref[:], sin_ref[:])

    for i in range(seq_len // q_block):
        @pl.when(step == i)
        def _(i=i):
            clear = i * q_block // 128 * 128
            keys = min(seq_len, -(-(i + 1) * q_block // 128) * 128)
            rows = pl.ds(i * q_block, q_block)
            cos_rows, sin_rows = cos_ref[rows, :], sin_ref[rows, :]
            row = lax.broadcasted_iota(jnp.int32, (q_block, keys - clear), 0) + i * q_block
            col = lax.broadcasted_iota(jnp.int32, (q_block, keys - clear), 1) + clear
            visible = row >= col
            q = jnp.concatenate([
                rotate(q_ref[:, g * HEAD_DIM:(g + 1) * HEAD_DIM].astype(jnp.float32), cos_rows, sin_rows)
                for g in range(group)])
            scores = lax.dot_general(q, kr_ref[:keys, :], (((1,), (1,)), ((), ())), preferred_element_type=jnp.float32)
            rounded = []
            for g in range(group):
                part = scores[g * q_block:(g + 1) * q_block]
                edge = jnp.where(visible, part[:, clear:], -1e30)
                part = edge if clear == 0 else jnp.concatenate([part[:, :clear], edge], axis=1)
                part = part * HEAD_DIM ** -0.5
                probs = jnp.exp(part - jnp.max(part, axis=-1, keepdims=True))
                rounded.append((probs * (1.0 / jnp.sum(probs, axis=-1, keepdims=True))).astype(jnp.bfloat16))
            mix = jnp.dot(jnp.concatenate(rounded), v_ref[:keys, :], preferred_element_type=jnp.float32).astype(jnp.bfloat16)
            for g in range(group):
                o_ref[:, g * HEAD_DIM:(g + 1) * HEAD_DIM] = mix[g * q_block:(g + 1) * q_block]


def attention(q, k, v, cos_t, sin_t, order):
    seq_len, kv_width = k.shape
    q_block = seq_len // 8
    group = q.shape[1] // kv_width
    wide = group * HEAD_DIM
    return pl.pallas_call(
        functools.partial(attention_kernel, q_block, group),
        grid_spec=pltpu.PrefetchScalarGridSpec(
            num_scalar_prefetch=1,
            grid=(kv_width // HEAD_DIM, 8),
            in_specs=[
                pl.BlockSpec((q_block, wide), lambda h, i, order_ref: (i, h)),
                pl.BlockSpec((seq_len, HEAD_DIM), lambda h, i, order_ref: (0, h)),
                pl.BlockSpec((seq_len, HEAD_DIM), lambda h, i, order_ref: (0, h)),
                pl.BlockSpec((seq_len, HEAD_DIM), lambda h, i, order_ref: (0, 0)),
                pl.BlockSpec((seq_len, HEAD_DIM), lambda h, i, order_ref: (0, 0)),
            ],
            out_specs=[
                pl.BlockSpec((q_block, wide), lambda h, i, order_ref: (order_ref[i], h)),
                pl.BlockSpec((seq_len, HEAD_DIM), lambda h, i, order_ref: (0, h)),
            ],
        ),
        out_shape=[jax.ShapeDtypeStruct(q.shape, jnp.bfloat16), jax.ShapeDtypeStruct(k.shape, jnp.bfloat16)],
        compiler_params=params(32),
        cost_estimate=cost(9_000_000_000, 5_000_000),
    )(order, q, k, v, cos_t, sin_t)


def project_kernel(request, next_request, embeds_hbm, moved_hbm, gain_ref, wq_ref, wk_ref, wv_ref, q_ref, k_ref, v_ref, own_ref, *rest):
    a, b, s = lax.axis_index('a'), lax.axis_index('b'), lax.axis_index('stage')
    if next_request is not None:
        next_hbm, x, normed, sems, send_sem, recv_sem = rest
        passed = pltpu.make_async_remote_copy(
            src_ref=embeds_hbm.at[0, next_request], dst_ref=next_hbm, send_sem=send_sem, recv_sem=recv_sem,
            device_id={'stage': 1 - s}, device_id_type=pl.DeviceIdType.MESH)
    else:
        x, normed, sems = rest
    step = pl.program_id(0)
    last = pl.num_programs(0) - 1
    pieces = sems.shape[0]
    rows = x.shape[0] // pieces
    block = own_ref.shape[0] // 2

    @pl.when(step == 0)
    def _():
        def fetch(source, i):
            return pltpu.make_async_copy(source.at[pl.ds(i * rows, rows)], x.at[pl.ds(i * rows, rows)], sems.at[i])

        @pl.when(s == 0)
        def _():
            for i in range(pieces):
                fetch(embeds_hbm.at[0, request], i).start()

        @pl.when(s == 1)
        def _():
            for i in range(pieces):
                fetch(moved_hbm, i).start()

        if next_request is not None:
            barrier = pltpu.get_barrier_semaphore()
            pl.semaphore_signal(barrier, inc=1, device_id={'stage': 1 - s}, device_id_type=pl.DeviceIdType.MESH)
            pl.semaphore_wait(barrier, 1)

            @pl.when(s == 0)
            def _():
                passed.start()

        for i in range(pieces):
            fetch(moved_hbm, i).wait()
            normed[pl.ds(i * rows, rows), :] = normalised(x[pl.ds(i * rows, rows), :].astype(jnp.float32), gain_ref)
        for i, own in enumerate((2 * a + b, 4 + 2 * b + a)):
            own_ref[i * block:(i + 1) * block, :] = x[pl.ds(pl.multiple_of(own * block, 32), block), :]

    @pl.when(step < last)
    def _():
        q_ref[:] = matmul(normed[:], wq_ref[0]).astype(jnp.bfloat16)

    @pl.when(step == last)
    def _():
        k_ref[:] = matmul(normed[:], wk_ref[0]).astype(jnp.bfloat16)
        v_ref[:] = matmul(normed[:], wv_ref[0]).astype(jnp.bfloat16)
        if next_request is not None:
            @pl.when(s == 0)
            def _():
                passed.wait_send()

            @pl.when(s == 1)
            def _():
                passed.wait_recv()


def projections(embeds, moved, request, next_request, gain, w_query, w_key, w_value):
    seq_len, width = moved.shape
    q_width, kv_width = w_query.shape[2], w_key.shape[2]
    tile = 2 * kv_width
    q_steps = q_width // tile
    hbm = pl.BlockSpec(memory_space=pltpu.HBM)

    def first(shape):
        return pl.BlockSpec(shape, lambda j: (0,) * len(shape))

    def bf16(*shape):
        return jax.ShapeDtypeStruct(shape, jnp.bfloat16)

    out_specs = [
        pl.BlockSpec((seq_len, tile), lambda j: (0, jnp.minimum(j, q_steps - 1))),
        first((seq_len, kv_width)), first((seq_len, kv_width)), first((seq_len // 4, width))]
    out_shape = [bf16(seq_len, q_width), bf16(seq_len, kv_width), bf16(seq_len, kv_width), bf16(seq_len // 4, width)]
    scratch = [pltpu.VMEM((seq_len, width), jnp.bfloat16), pltpu.VMEM((seq_len, width), jnp.bfloat16), pltpu.SemaphoreType.DMA((4,))]
    extra = {}
    if next_request is not None:
        out_specs.append(hbm)
        out_shape.append(bf16(seq_len, width))
        scratch += [pltpu.SemaphoreType.DMA, pltpu.SemaphoreType.DMA]
        extra = dict(collective_id=1 + request, has_side_effects=True)
    return pl.pallas_call(
        functools.partial(project_kernel, request, next_request),
        grid=(q_steps + 1,),
        in_specs=[
            hbm, hbm, first((1, width)),
            pl.BlockSpec((1, width, tile), lambda j: (0, 0, jnp.minimum(j, q_steps - 1))),
            first((1, width, kv_width)), first((1, width, kv_width)),
        ],
        out_specs=out_specs,
        out_shape=out_shape,
        scratch_shapes=scratch,
        compiler_params=params(56, **extra),
        cost_estimate=cost(10_000_000_000, 30_000_000),
    )(embeds, moved, gain, w_query, w_key, w_value)


def gate_up_kernel(own_hbm, near_1_hbm, near_2_hbm, far_1_hbm, far_2_hbm, wg_ref, wu_ref, o_ref, rows, sems):
    block = near_1_hbm.shape[0]

    @pl.when(pl.program_id(0) == 0)
    def _():
        copies = []
        for i, (source, start) in enumerate((
                (own_hbm.at[pl.ds(0, block)], 0), (near_1_hbm, block), (far_1_hbm, 2 * block),
                (own_hbm.at[pl.ds(block, block)], 4 * block), (near_2_hbm, 5 * block), (far_2_hbm, 6 * block))):
            copies.append(pltpu.make_async_copy(source, rows.at[pl.ds(start, source.shape[0])], sems.at[i]))
            copies[-1].start()
        for copy in copies:
            copy.wait()

    gate = jnp.dot(rows[:], wg_ref[0], preferred_element_type=jnp.float32).astype(jnp.bfloat16).astype(jnp.float32)
    up = jnp.dot(rows[:], wu_ref[0], preferred_element_type=jnp.float32).astype(jnp.bfloat16).astype(jnp.float32)
    o_ref[:] = gated(gate, up)


def gate_up(own, near_1, near_2, far_1, far_2, w_gate, w_up, first, count, tile):
    block, width = near_1.shape
    hbm = pl.BlockSpec(memory_space=pltpu.HBM)
    weight = pl.BlockSpec((1, width, tile), lambda j: (0, 0, first + j))
    return pl.pallas_call(
        gate_up_kernel,
        grid=(count,),
        in_specs=[hbm] * 5 + [weight] * 2,
        out_specs=pl.BlockSpec((8 * block, tile), lambda j: (0, j)),
        out_shape=jax.ShapeDtypeStruct((8 * block, count * tile), jnp.bfloat16),
        scratch_shapes=[pltpu.VMEM((8 * block, width), jnp.bfloat16), pltpu.SemaphoreType.DMA((6,))],
        compiler_params=params(56),
        cost_estimate=cost(32 * block * width * count * tile, 4 * width * count * tile),
    )(own, near_1, near_2, far_1, far_2, w_gate, w_up)


def down_kernel(act_1_ref, act_2_ref, w_ref, *o_refs):
    cut = act_1_ref.shape[1]
    product = jnp.dot(act_1_ref[:], w_ref[0, :cut, :], preferred_element_type=jnp.float32)
    product = (product + jnp.dot(act_2_ref[:], w_ref[0, cut:, :], preferred_element_type=jnp.float32)).astype(jnp.bfloat16)
    rows = o_refs[0].shape[0]
    for i, o_ref in enumerate(o_refs):
        o_ref[:] = product[i * rows:(i + 1) * rows]


def down(act_1, act_2, w_down, tile):
    rows, depth = act_1.shape[0], w_down.shape[1]
    width = w_down.shape[2]
    return pl.pallas_call(
        down_kernel,
        grid=(width // tile,),
        in_specs=[pl.BlockSpec(act_1.shape, lambda j: (0, 0)), pl.BlockSpec(act_2.shape, lambda j: (0, 0)),
                  pl.BlockSpec((1, depth, tile), lambda j: (0, 0, j))],
        out_specs=[pl.BlockSpec((rows // 4, tile), lambda j: (0, j))] * 4,
        out_shape=[jax.ShapeDtypeStruct((rows // 4, width), jnp.bfloat16)] * 4,
        compiler_params=params(56),
        cost_estimate=cost(2 * rows * depth * width, 2 * depth * width),
    )(act_1, act_2, w_down)


def kv_kernel(part_ref, x_ref, gain_ref, cos_ref, sin_ref, *refs):
    mine, other, o_ref, normed = refs[:8], refs[8:16], refs[16], refs[17]
    depth, columns = mine[0].shape
    half = 2 * depth
    whole = normalised(x_ref[:].astype(jnp.float32), gain_ref)
    normed[0] = whole[:, :half]
    normed[1] = whole[:, half:]
    part = part_ref[0]
    for piece in range(4):
        product = jnp.dot(normed[part, :, :depth], mine[2 * piece][:], preferred_element_type=jnp.float32)
        product += jnp.dot(normed[part, :, depth:], mine[2 * piece + 1][:], preferred_element_type=jnp.float32)
        product += jnp.dot(normed[1 - part, :, :depth], other[2 * piece][:], preferred_element_type=jnp.float32)
        product += jnp.dot(normed[1 - part, :, depth:], other[2 * piece + 1][:], preferred_element_type=jnp.float32)
        rounded = product.astype(jnp.bfloat16)
        base = piece * columns
        for h in range(columns // 2 // HEAD_DIM):
            cols = slice(h * HEAD_DIM, (h + 1) * HEAD_DIM)
            o_ref[:, base + h * HEAD_DIM:base + (h + 1) * HEAD_DIM] = rotate(rounded[:, cols].astype(jnp.float32), cos_ref[:], sin_ref[:])
        o_ref[:, base + columns // 2:base + columns] = rounded[:, columns // 2:]


def keys_values(x, gain, mine, other, cos_rows, sin_rows, part):
    rows, _ = x.shape
    depth, columns = mine[0].shape
    vmem = pl.BlockSpec(memory_space=pltpu.VMEM)
    return pl.pallas_call(
        kv_kernel,
        in_specs=[pl.BlockSpec(memory_space=pltpu.SMEM)] + [vmem] * 20,
        out_specs=vmem,
        out_shape=jax.ShapeDtypeStruct((rows, 4 * columns), jnp.bfloat16),
        scratch_shapes=[pltpu.VMEM((2, rows, 2 * depth), jnp.bfloat16)],
        compiler_params=params(40),
        cost_estimate=cost(32 * rows * depth * columns, 32 * depth * columns),
    )(part, x, gain, cos_rows, sin_rows, *mine, *other)


def tail_kernel(kv_heads, x0_ref, x1_ref, x2_ref, kv0_ref, kv1_ref, kv2_ref, gain_a_ref, gain_m_ref, cos_ref, sin_ref,
                wq_hbm, wo_hbm, wg_hbm, wu_hbm, wd_hbm, o_ref,
                wq, wo, wg, wu, wd, x_src, x_all, q_src, q_all, pk_src, pk_all, mix, p_src, p_all, r_src, r_all,
                w_sem, x_send, x_recv, q_send, q_recv, pk_send, pk_recv, p_send, p_recv, r_send, r_recv):
    a, b, s = lax.axis_index('a'), lax.axis_index('b'), lax.axis_index('stage')
    me = 4 * b + 2 * a + s
    x_refs, kv_refs = (x0_ref, x1_ref, x2_ref), (kv0_ref, kv1_ref, kv2_ref)
    n_chunk = len(x_refs)
    n_rows = o_ref.shape[0]
    group = wq.shape[1] // HEAD_DIM
    eighth, wide = wq.shape[1], wg.shape[1]

    cuts = [
        (wq_hbm.at[1, :, pl.ds(pl.multiple_of(s * eighth, eighth), eighth)], wq),
        (wo_hbm.at[1, pl.ds(pl.multiple_of(s * eighth, eighth), eighth), :], wo),
        (wg_hbm.at[1, :, pl.ds(pl.multiple_of(s * wide, wide), wide)], wg),
        (wu_hbm.at[1, :, pl.ds(pl.multiple_of(s * wide, wide), wide)], wu),
        (wd_hbm.at[1, pl.ds(pl.multiple_of(s * wide, wide), wide), :], wd),
    ]
    fetches = [pltpu.make_async_copy(src, dst, w_sem.at[i]) for i, (src, dst) in enumerate(cuts)]
    for fetch in fetches:
        fetch.start()

    peers = []
    for d in range(1, 8):
        peer_b = 1 - b if d & 4 else b
        peer_a = 1 - a if d & 2 else a
        peer_s = 1 - s if d & 1 else s
        peers.append((4 * peer_b + 2 * peer_a + peer_s, {'b': peer_b, 'a': peer_a, 'stage': peer_s}))

    barrier = pltpu.get_barrier_semaphore()
    for _, where in peers:
        pl.semaphore_signal(barrier, inc=1, device_id=where, device_id_type=pl.DeviceIdType.MESH)
    pl.semaphore_wait(barrier, 7)

    def exchange(source_of, everyone, send, recv):
        copies = [
            pltpu.make_async_remote_copy(
                src_ref=source_of(peer), dst_ref=everyone.at[me], send_sem=send.at[i], recv_sem=recv.at[i],
                device_id=where, device_id_type=pl.DeviceIdType.MESH)
            for i, (peer, where) in enumerate(peers)]
        arrivals = [
            pltpu.make_async_remote_copy(
                src_ref=source_of(peer), dst_ref=everyone.at[peer], send_sem=send.at[i], recv_sem=recv.at[i],
                device_id=where, device_id_type=pl.DeviceIdType.MESH)
            for i, (peer, where) in enumerate(peers)]
        for copy in copies:
            copy.start()
        everyone[me] = source_of(me)[:]
        for arrival in arrivals:
            arrival.wait_recv()
        for copy in copies:
            copy.wait_send()

    row_index = lax.broadcasted_iota(jnp.int32, (n_rows, x0_ref.shape[1]), 0)
    rows = jnp.zeros((n_rows, x0_ref.shape[1]), jnp.float32)
    for c in range(n_chunk):
        last_row = x_refs[c][x_refs[c].shape[0] - 1:, :].astype(jnp.float32)
        rows = jnp.where(row_index == n_chunk * s + c, last_row, rows)
    x_src[:] = rows.astype(jnp.bfloat16)
    is_owner = a + b == 2

    def x_copy(i):
        return pltpu.make_async_remote_copy(
            src_ref=x_src, dst_ref=x_all.at[s], send_sem=x_send.at[i], recv_sem=x_recv.at[s],
            device_id=peers[i][1], device_id_type=pl.DeviceIdType.MESH)

    @pl.when(is_owner)
    def _():
        for i in range(7):
            x_copy(i).start()
        x_all[s] = x_src[:]

    for o in range(2):
        @pl.when(me != 6 + o)
        def _(o=o):
            pltpu.make_async_remote_copy(
                src_ref=x_src, dst_ref=x_all.at[o], send_sem=x_send.at[0], recv_sem=x_recv.at[o],
                device_id=peers[0][1], device_id_type=pl.DeviceIdType.MESH).wait_recv()

    @pl.when(is_owner)
    def _():
        for i in range(7):
            x_copy(i).wait_send()

    last = x_all[0].astype(jnp.float32) + x_all[1].astype(jnp.float32)
    fetches[0].wait()
    q = jnp.dot(normalised(last, gain_a_ref), wq[:], preferred_element_type=jnp.float32)
    q_src[:] = q.astype(jnp.bfloat16).astype(jnp.float32)
    exchange(lambda peer: q_src, q_all, q_send, q_recv)

    kv_width = kv_heads * HEAD_DIM
    for piece in range(4):
        head_b = 1 - b if piece & 2 else b
        head_a = 1 - a if piece & 1 else a
        for h in range(kv_heads):
            head = (2 * head_b + head_a) * kv_heads + h
            low = 2 * piece * kv_width + h * HEAD_DIM
            for c in range(n_chunk):
                q_row = q_all[head, pl.ds(n_chunk * s + c, 1), :]
                q_heads = jnp.concatenate([q_row[:, g * HEAD_DIM:(g + 1) * HEAD_DIM] for g in range(group)])
                q_heads = rotate(q_heads, cos_ref[:], sin_ref[:])
                k = kv_refs[c][:, low:low + HEAD_DIM]
                v = kv_refs[c][:, low + kv_width:low + kv_width + HEAD_DIM]
                scores = lax.dot_general(q_heads, k, (((1,), (1,)), ((), ())), preferred_element_type=jnp.float32) * HEAD_DIM ** -0.5
                top = jnp.max(scores, axis=-1, keepdims=True)
                probs = jnp.exp(scores - top)
                total = jnp.sum(probs, axis=-1, keepdims=True)
                pk_src[head, c, :, :HEAD_DIM] = jnp.dot(probs.astype(jnp.bfloat16), v, preferred_element_type=jnp.float32)
                pk_src[head, c, :, HEAD_DIM:2 * HEAD_DIM] = jnp.broadcast_to(top, (group, HEAD_DIM))
                pk_src[head, c, :, 2 * HEAD_DIM:] = jnp.broadcast_to(total, (group, HEAD_DIM))
    exchange(lambda peer: pk_src.at[peer], pk_all, pk_send, pk_recv)

    mix[:] = jnp.zeros_like(mix)
    for stage in range(2):
        for c in range(n_chunk):
            found = [pk_all[2 * i + stage, c] for i in range(4)]
            top = found[0][:, HEAD_DIM:2 * HEAD_DIM]
            for part in found[1:]:
                top = jnp.maximum(top, part[:, HEAD_DIM:2 * HEAD_DIM])
            value, total = jnp.zeros_like(top), jnp.zeros_like(top)
            for part in found:
                scale = jnp.exp(part[:, HEAD_DIM:2 * HEAD_DIM] - top)
                value += part[:, :HEAD_DIM] * scale
                total += part[:, 2 * HEAD_DIM:] * scale
            value = value / total
            for g in range(group):
                mix[n_chunk * stage + c:n_chunk * stage + c + 1, g * HEAD_DIM:(g + 1) * HEAD_DIM] = value[g:g + 1, :]

    def summed(everyone):
        total = everyone[0].astype(jnp.float32)
        for i in range(1, 8):
            total += everyone[i].astype(jnp.float32)
        return total.astype(jnp.bfloat16).astype(jnp.float32)

    fetches[1].wait()
    p_src[:] = jnp.dot(mix[:].astype(jnp.bfloat16), wo[:], preferred_element_type=jnp.float32).astype(jnp.bfloat16)
    exchange(lambda peer: p_src, p_all, p_send, p_recv)
    last = (last + summed(p_all)).astype(jnp.bfloat16).astype(jnp.float32)
    normed = normalised(last, gain_m_ref)
    fetches[2].wait()
    gate = jnp.dot(normed, wg[:], preferred_element_type=jnp.float32).astype(jnp.bfloat16).astype(jnp.float32)
    fetches[3].wait()
    up = jnp.dot(normed, wu[:], preferred_element_type=jnp.float32).astype(jnp.bfloat16).astype(jnp.float32)
    act = gated(gate, up)
    fetches[4].wait()
    r_src[:] = jnp.dot(act, wd[:], preferred_element_type=jnp.float32).astype(jnp.bfloat16)
    exchange(lambda peer: r_src, r_all, r_send, r_recv)
    o_ref[:] = (last + summed(r_all)).astype(jnp.bfloat16)


def last_rows(finals, kvs, gain_a, gain_m, cos_row, sin_row, w_query, w_out, w_gate, w_up, w_down, kv_heads):
    width = finals[0].shape[1]
    eighth = w_query.shape[2] // 2
    wide = w_gate.shape[2] // 2
    group = eighth // HEAD_DIM
    n_rows = 8
    n_chunk = len(finals)
    vmem = pl.BlockSpec(memory_space=pltpu.VMEM)
    last_block = pl.BlockSpec((n_rows, width), lambda i: (finals[0].shape[0] // n_rows - 1, 0))

    def full(value):
        return pl.BlockSpec(value.shape, lambda i: (0,) * value.ndim)

    seven = pltpu.SemaphoreType.DMA((7,))
    return pl.pallas_call(
        functools.partial(tail_kernel, kv_heads),
        grid=(1,),
        in_specs=[last_block] * n_chunk + [full(kv) for kv in kvs] + [full(v) for v in (gain_a, gain_m, cos_row, sin_row)]
        + [pl.BlockSpec(memory_space=pl.ANY)] * 5,
        out_specs=pl.BlockSpec((n_rows, width), lambda i: (0, 0)),
        out_shape=jax.ShapeDtypeStruct((n_rows, width), jnp.bfloat16),
        scratch_shapes=[
            pltpu.VMEM((width, eighth), jnp.bfloat16),
            pltpu.VMEM((eighth, width), jnp.bfloat16),
            pltpu.VMEM((width, wide), jnp.bfloat16),
            pltpu.VMEM((width, wide), jnp.bfloat16),
            pltpu.VMEM((wide, width), jnp.bfloat16),
            pltpu.VMEM((n_rows, width), jnp.bfloat16),
            pltpu.VMEM((2, n_rows, width), jnp.bfloat16),
            pltpu.VMEM((n_rows, eighth), jnp.float32),
            pltpu.VMEM((8, n_rows, eighth), jnp.float32),
            pltpu.VMEM((8, n_chunk, group, 3 * HEAD_DIM), jnp.float32),
            pltpu.VMEM((8, n_chunk, group, 3 * HEAD_DIM), jnp.float32),
            pltpu.VMEM((n_rows, eighth), jnp.float32),
            pltpu.VMEM((n_rows, width), jnp.bfloat16),
            pltpu.VMEM((8, n_rows, width), jnp.bfloat16),
            pltpu.VMEM((n_rows, width), jnp.bfloat16),
            pltpu.VMEM((8, n_rows, width), jnp.bfloat16),
            pltpu.SemaphoreType.DMA((5,)),
            seven, pltpu.SemaphoreType.DMA((2,)), seven, seven, seven, seven, seven, seven, seven, seven,
        ],
        compiler_params=params(63, collective_id=0, has_side_effects=True),
        cost_estimate=cost(9_000_000_000, 60_000_000),
    )(*finals, *kvs, gain_a, gain_m, cos_row, sin_row, w_query, w_out, w_gate, w_up, w_down)


def write_heads(k_ref, v_ref, low, high):
    rows, kv2 = low.shape
    for ref, start in ((k_ref, 0), (v_ref, kv2 // 2)):
        heads = jnp.concatenate([low[:, start:start + kv2 // 2], high[:, start:start + kv2 // 2]], axis=1)
        ref[0, 0, 0] = heads.reshape(rows, kv2 // HEAD_DIM, HEAD_DIM)


def first_cut_kernel(where_ref, near_ref, far_ref, k_ref, v_ref):
    own_low = where_ref[0] == 0
    near, far = near_ref[0], far_ref[0]
    write_heads(k_ref, v_ref, jnp.where(own_low, near, far), jnp.where(own_low, far, near))


def first_cut(near, far, where):
    n_chunk, seq_len, columns = near.shape
    rows = seq_len // 2
    heads = columns // HEAD_DIM
    source = pl.BlockSpec((1, rows, columns), lambda c, j, where_ref: (c, j, 0))
    target = pl.BlockSpec((1, 1, 1, rows, heads, HEAD_DIM), lambda c, j, where_ref: (0, 0, c, j, 0, 0))
    return pl.pallas_call(
        first_cut_kernel,
        grid_spec=pltpu.PrefetchScalarGridSpec(num_scalar_prefetch=1, grid=(n_chunk, 2), in_specs=[source] * 2, out_specs=[target] * 2),
        out_shape=[jax.ShapeDtypeStruct((1, 2, n_chunk, seq_len, heads, HEAD_DIM), jnp.bfloat16)] * 2,
        compiler_params=params(32),
        cost_estimate=cost(1_000_000_000, 19_000_000),
    )(where, near, far)


def second_cut_kernel(where_ref, near_ref, far_ref, k_in, v_in, k_ref, v_ref):
    columns = near_ref.shape[-1] // 2

    def put(source):
        mine, other = source[:, :columns], source[:, columns:]
        own_low = where_ref[0] + pl.program_id(0) - 2 * where_ref[0] * pl.program_id(0) == 0
        write_heads(k_ref, v_ref, jnp.where(own_low, mine, other), jnp.where(own_low, other, mine))

    @pl.when(pl.program_id(0) == 0)
    def _():
        put(near_ref[0])

    @pl.when(pl.program_id(0) == 1)
    def _():
        put(far_ref[0])


def second_cut(near, far, where, k_cache, v_cache, request):
    _, rows, columns = near.shape
    block = rows // 2
    heads = columns // 2 // HEAD_DIM

    def place(i, j, half, where_ref):
        along_x = where_ref[0] + i - 2 * where_ref[0] * i
        along_y = where_ref[1] + j - 2 * where_ref[1] * j
        return 0, 1, request, (1 - half) * (2 * along_x + along_y) + half * (4 + 2 * along_y + along_x), 0, 0

    source = pl.BlockSpec((1, block, columns), lambda i, j, half, where_ref: (j, half, 0))
    target = pl.BlockSpec((1, 1, 1, block, heads, HEAD_DIM), place)
    whole = pl.BlockSpec(memory_space=pl.ANY)
    return pl.pallas_call(
        second_cut_kernel,
        grid_spec=pltpu.PrefetchScalarGridSpec(
            num_scalar_prefetch=1, grid=(2, 2, 2), in_specs=[source] * 2 + [whole] * 2, out_specs=[target] * 2),
        out_shape=[jax.ShapeDtypeStruct(k_cache.shape, jnp.bfloat16)] * 2,
        input_output_aliases={3: 0, 4: 1},
        compiler_params=params(32),
        cost_estimate=cost(300_000_000, 5_000_000),
    )(where, near, far, k_cache, v_cache)


def solution(mesh):
    tp_axes = ('b', 'a')
    weight_cols = P(None, None, tp_axes)
    weight_rows = P(None, tp_axes, None)
    in_specs = (P('stage', 'dp', None, None), P(), weight_cols, weight_cols, weight_cols, weight_rows, P(), weight_cols, weight_cols, weight_rows)
    cache_spec = P('stage', None, ('dp', 'a'), None, 'b', None)
    out_specs = (cache_spec, cache_spec, P('stage', ('dp', 'a'), None))

    def over_x(value):
        return lax.ppermute(value, 'a', SWAP)

    def over_y(value):
        return lax.ppermute(value, 'b', SWAP)

    def across(value):
        return lax.ppermute(value, 'stage', SWAP)

    def hold(values, *after):
        return lax.optimization_barrier((values, after))[0]

    def stage_program(embeds, attn_gain, w_query, w_key, w_value, w_out, mlp_gain, w_gate, w_up, w_down):
        a, b, s = lax.axis_index('a'), lax.axis_index('b'), lax.axis_index('stage')
        n_req, seq_len, width = embeds.shape[1:]
        n_chunk = n_req // 2
        block = seq_len // 8
        kv_width = w_key.shape[2]
        kv_heads = kv_width // HEAD_DIM
        kv2 = 2 * kv_width
        half_rows = seq_len // 2
        half_width = width // 2
        cos_t, sin_t = rope_tables(seq_len)
        chip = 2 * b + a
        part = s.astype(jnp.int32).reshape(1)
        where = jnp.stack([a, b]).astype(jnp.int32)

        fours = jnp.arange(4, dtype=jnp.int32)
        order = jnp.concatenate([jnp.bitwise_xor(fours, 2 * a + b), 4 + jnp.bitwise_xor(fours, chip)]).astype(jnp.int32)

        def own_rows(value):
            return jnp.concatenate([
                lax.dynamic_slice_in_dim(value, block * (2 * a + b), block, 0),
                lax.dynamic_slice_in_dim(value, half_rows + block * chip, block, 0)])

        def quarters(part_sum):
            return [part_sum[2 * i * block:2 * (i + 1) * block] for i in range(4)]

        def send_parts(parts):
            return parts[1], parts[3]

        def send_wide(sends):
            return over_x(sends[0]), over_y(sends[1])

        def add_wide(parts, got):
            return add_rounded(parts[0], got[0]), add_rounded(parts[2], got[1])

        def send_narrow(sums):
            return over_y(sums[0][block:]), over_x(sums[1][block:])

        def add_narrow(residual, sums, got):
            kept = jnp.concatenate([sums[0][:block], sums[1][:block]])
            return add_rounded(residual, add_rounded(kept, jnp.concatenate(got)))

        def gather_near(own):
            return over_y(own[:block]), over_x(own[block:])

        def join_near(own, got):
            return jnp.concatenate([own[:block], got[0]]), jnp.concatenate([own[block:], got[1]])

        def gather_far(near):
            return over_x(near[0]), over_y(near[1])

        def take(value):
            return lax.ppermute(value, 'stage', [(0, 1)])

        moved0 = take(embeds[0, n_chunk])

        quarter_width = width // 4

        def w_block(half, lower):
            rows = half * half_width + lower * quarter_width
            return jnp.concatenate([lax.dynamic_slice_in_dim(w[1], rows, quarter_width, 0) for w in (w_key, w_value)], axis=1)

        w_top, w_bottom = hold((w_block(s, 0), w_block(s, 1)), embeds[0, n_chunk, :8, :128])
        top_y, bottom_x = over_y(w_top), over_x(w_bottom)
        top_x, bottom_y = over_x(w_top), over_y(w_bottom)

        def project(moved, request):
            following = n_chunk + request + 1 if request + 1 < n_chunk else None
            q, k, v, own, *passed = projections(embeds, moved, request, following, attn_gain[:1], w_query, w_key, w_value)
            return (q, k, v), own, passed

        def attend(qkv):
            mix, k_rot = attention(*qkv, cos_t, sin_t, order)
            return mix, jnp.concatenate([k_rot, qkv[2]], axis=1)

        def out_of(mix):
            return quarters(matmul(mix, w_out[0]).astype(jnp.bfloat16))

        mlp_tile = 512
        n_tiles = w_gate.shape[2] // mlp_tile
        first_tiles = n_tiles // 2

        def act_of(h, got, far, second):
            start, count = (first_tiles, n_tiles - first_tiles) if second else (0, first_tiles)
            return gate_up(h, got[0], got[1], far[0], far[1], w_gate, w_up, start, count, mlp_tile)

        def down_of(act_1, act_2):
            return down(act_1, act_2, w_down, mlp_tile)

        own_cos, own_sin = own_rows(cos_t), own_rows(sin_t)

        qkv0, own_x0, (moved1,) = project(moved0, 0)
        top_d, bottom_d = over_x(hold(top_y, qkv0)), over_y(hold(bottom_x, qkv0))
        mix0, kv0_0 = attend(qkv0)
        p0 = out_of(mix0)
        send = send_parts(p0)
        wide0 = send_wide(send)

        qkv1, own_x1, (moved2,) = project(hold(moved1, send), 1)
        sums0 = add_wide(p0, hold(wide0, qkv1))
        narrow0 = send_narrow(sums0)
        mix1, kv0_1 = attend(hold(qkv1, sums0))
        own1_0 = add_narrow(own_x0, sums0, hold(narrow0, mix1))
        h0 = rms_norm(own1_0, mlp_gain[0])
        near_got0 = gather_near(h0)
        p1 = out_of(hold(mix1, h0))
        send = send_parts(p1)
        wide1 = send_wide(send)
        near0 = join_near(h0, hold(near_got0, send))
        far0 = gather_far(near0)

        qkv2, own_x2, _ = project(hold(moved2, near0), 2)
        mix2, kv0_2 = attend(qkv2)
        sums1 = add_wide(p1, hold(wide1, mix2))
        narrow1 = send_narrow(sums1)
        p2 = out_of(hold(mix2, sums1))
        send = send_parts(p2)
        wide2 = send_wide(send)

        rows = (h0, near_got0, hold(far0, send))
        gate = act_of(*rows, False)
        own1_1 = add_narrow(own_x1, sums1, hold(narrow1, gate))
        h1 = rms_norm(own1_1, mlp_gain[0])
        near_got1 = gather_near(h1)
        act = act_of(*hold(rows, h1), True)
        near1 = join_near(h1, hold(near_got1, act))
        far1 = gather_far(near1)
        sums2 = add_wide(p2, hold(wide2, near1))
        narrow2 = send_narrow(sums2)
        d0 = down_of(gate, hold(act, sums2))
        send = send_parts(d0)
        wide0 = send_wide(send)

        fetched = hold((top_x, bottom_x, top_y, bottom_y, top_d, bottom_d), send)
        w_mine = [w_top, w_bottom] + list(fetched)
        w_other = [w_block(1 - s, 0), w_block(1 - s, 1)] + [across(piece) for piece in fetched]

        rows = (h1, near_got1, hold(far1, send))
        gate = act_of(*rows, False)
        own1_2 = add_narrow(own_x2, sums2, hold(narrow2, gate))
        h2 = rms_norm(own1_2, mlp_gain[0])
        near_got2 = gather_near(h2)
        act = act_of(*hold(rows, h2), True)
        near2 = join_near(h2, hold(near_got2, act))
        far2 = gather_far(near2)
        sums0 = add_wide(d0, hold(wide0, near2))
        narrow0 = send_narrow(sums0)
        d1 = down_of(gate, hold(act, sums0))
        send = send_parts(d1)
        wide1 = send_wide(send)

        def keys_values_of(final):
            return keys_values(final, attn_gain[1:2], w_mine, w_other, own_cos, own_sin, part)

        def to_decode(value):
            return lax.ppermute(value, ('a', 'stage'), FROM_NEAR), lax.ppermute(value, ('a', 'stage'), FROM_FAR)

        def along_y(kv, *after):
            return over_y(hold(kv[:, 2 * kv2:], *after))

        def to_decode_rows(kv, got):
            return to_decode(jnp.stack([kv[:, :2 * kv2], got]))

        rows = (h2, near_got2, hold(far2, send))
        gate = act_of(*rows, False)
        final0 = add_narrow(own1_0, sums0, hold(narrow0, gate))
        kv1_0 = keys_values_of(final0)
        got_0 = along_y(kv1_0)
        cut0 = to_decode(hold(jnp.stack([kv0_0, kv0_1, kv0_2]), kv1_0))
        act = act_of(*hold(rows, kv1_0), True)
        sums1 = add_wide(d1, hold(wide1, act))
        narrow1 = send_narrow(sums1)
        cut1_0 = to_decode_rows(kv1_0, hold(got_0, sums1))
        d2 = down_of(gate, hold(act, sums1))
        send = send_parts(d2)
        wide2 = send_wide(send)
        final1 = add_narrow(own1_1, sums1, hold(narrow1, send))
        kv1_1 = keys_values_of(final1)
        got_1 = along_y(kv1_1)
        k_cache, v_cache = first_cut(*hold(cut0, kv1_1), where)
        sums2 = add_wide(d2, hold(wide2, k_cache))
        narrow2 = send_narrow(sums2)
        k_cache, v_cache = second_cut(*hold(cut1_0, sums2), where, k_cache, v_cache, 0)
        final2 = add_narrow(own1_2, sums2, hold(narrow2, k_cache))
        kv1_2 = keys_values_of(final2)
        got_2 = along_y(kv1_2)
        cut1_1 = to_decode_rows(kv1_1, hold(got_1, kv1_2))
        cut1_2 = to_decode_rows(kv1_2, got_2)

        last = last_rows(
            (final0, final1, final2), (kv1_0, kv1_1, hold(kv1_2, got_2)), attn_gain[1:2], mlp_gain[1:2],
            cos_t[-1:], sin_t[-1:], w_query, w_out, w_gate, w_up, w_down, kv_heads)
        last_out = lax.dynamic_slice_in_dim(last, a * n_chunk, n_chunk, 0)
        last_out = jnp.where(s == 1, last_out, jnp.zeros_like(last_out))

        for c, cut in ((1, cut1_1), (2, cut1_2)):
            k_cache, v_cache = second_cut(*hold(cut, last), where, k_cache, v_cache, c)
        return k_cache, v_cache, last_out[None]

    return jax.shard_map(stage_program, mesh=mesh, in_specs=in_specs, out_specs=out_specs, check_vma=False)
```

```python
import functools

import jax
import jax.numpy as jnp
from jax import lax
from jax.experimental import pallas as pl
from jax.experimental.pallas import tpu as pltpu
from jax.sharding import PartitionSpec as P


HEAD_DIM = 128
ROPE_BASE = 500000.0
NORM_EPS = 1e-5
MIB = 1 << 20
SWAP = [(0, 1), (1, 0)]
FROM_FAR = [(2, 1), (1, 3)]
FROM_NEAR = [(0, 1), (3, 3)]


def rms_norm(hidden, gain_vec):
    as_f32 = hidden.astype(jnp.float32)
    inv_rms = lax.rsqrt(jnp.mean(as_f32 * as_f32, axis=-1, keepdims=True) + NORM_EPS)
    return (as_f32 * inv_rms * gain_vec).astype(jnp.bfloat16)


def rope_tables(seq_len):
    half_dim = HEAD_DIM // 2
    inv_freq = ROPE_BASE ** (-2.0 * jnp.arange(half_dim, dtype=jnp.float32) / HEAD_DIM)
    angles = jnp.arange(seq_len, dtype=jnp.float32)[:, None] * inv_freq[None, :]
    cos_t, sin_t = jnp.cos(angles), jnp.sin(angles)
    return jnp.concatenate([cos_t, cos_t], axis=-1), jnp.concatenate([-sin_t, sin_t], axis=-1)


def matmul(left, right):
    return jnp.dot(left, right, preferred_element_type=jnp.float32)


def params(mebibytes, **extra):
    return pltpu.CompilerParams(vmem_limit_bytes=mebibytes * MIB, **extra)


def cost(flops, bytes_accessed):
    return pl.CostEstimate(flops=flops, bytes_accessed=bytes_accessed, transcendentals=0)


def normalised(as_f32, gain_ref):
    inv_rms = lax.rsqrt(jnp.mean(as_f32 * as_f32, axis=-1, keepdims=True) + NORM_EPS)
    return (as_f32 * inv_rms * gain_ref[:]).astype(jnp.bfloat16)


def gated(gate, up):
    return (gate * (1.0 / (1.0 + jnp.exp(-gate))) * up).astype(jnp.bfloat16)


def add_rounded(left, right):
    return (left.astype(jnp.float32) + right.astype(jnp.float32)).astype(jnp.bfloat16)


def rotate(as_f32, cos_rows, sin_rows):
    return (as_f32 * cos_rows + pltpu.roll(as_f32, HEAD_DIM // 2, 1) * sin_rows).astype(jnp.bfloat16)


def attention_kernel(q_block, group, _, q_ref, k_ref, v_ref, cos_ref, sin_ref, o_ref, kr_ref):
    step = pl.program_id(1)
    seq_len = k_ref.shape[0]

    @pl.when(step == 0)
    def _():
        kr_ref[:] = rotate(k_ref[:].astype(jnp.float32), cos_ref[:], sin_ref[:])

    for i in range(seq_len // q_block):
        @pl.when(step == i)
        def _(i=i):
            clear = i * q_block // 128 * 128
            keys = min(seq_len, -(-(i + 1) * q_block // 128) * 128)
            rows = pl.ds(i * q_block, q_block)
            cos_rows, sin_rows = cos_ref[rows, :], sin_ref[rows, :]
            row = lax.broadcasted_iota(jnp.int32, (q_block, keys - clear), 0) + i * q_block
            col = lax.broadcasted_iota(jnp.int32, (q_block, keys - clear), 1) + clear
            visible = row >= col
            q = jnp.concatenate([
                rotate(q_ref[:, g * HEAD_DIM:(g + 1) * HEAD_DIM].astype(jnp.float32), cos_rows, sin_rows)
                for g in range(group)])
            scores = lax.dot_general(q, kr_ref[:keys, :], (((1,), (1,)), ((), ())), preferred_element_type=jnp.float32)
            rounded = []
            for g in range(group):
                part = scores[g * q_block:(g + 1) * q_block]
                edge = jnp.where(visible, part[:, clear:], -1e30)
                part = edge if clear == 0 else jnp.concatenate([part[:, :clear], edge], axis=1)
                part = part * HEAD_DIM ** -0.5
                probs = jnp.exp(part - jnp.max(part, axis=-1, keepdims=True))
                rounded.append((probs * (1.0 / jnp.sum(probs, axis=-1, keepdims=True))).astype(jnp.bfloat16))
            mix = jnp.dot(jnp.concatenate(rounded), v_ref[:keys, :], preferred_element_type=jnp.float32).astype(jnp.bfloat16)
            for g in range(group):
                o_ref[:, g * HEAD_DIM:(g + 1) * HEAD_DIM] = mix[g * q_block:(g + 1) * q_block]


def attention(q, k, v, cos_t, sin_t, order):
    seq_len, kv_width = k.shape
    q_block = seq_len // 8
    group = q.shape[1] // kv_width
    wide = group * HEAD_DIM
    return pl.pallas_call(
        functools.partial(attention_kernel, q_block, group),
        grid_spec=pltpu.PrefetchScalarGridSpec(
            num_scalar_prefetch=1,
            grid=(kv_width // HEAD_DIM, 8),
            in_specs=[
                pl.BlockSpec((q_block, wide), lambda h, i, order_ref: (i, h)),
                pl.BlockSpec((seq_len, HEAD_DIM), lambda h, i, order_ref: (0, h)),
                pl.BlockSpec((seq_len, HEAD_DIM), lambda h, i, order_ref: (0, h)),
                pl.BlockSpec((seq_len, HEAD_DIM), lambda h, i, order_ref: (0, 0)),
                pl.BlockSpec((seq_len, HEAD_DIM), lambda h, i, order_ref: (0, 0)),
            ],
            out_specs=[
                pl.BlockSpec((q_block, wide), lambda h, i, order_ref: (order_ref[i], h)),
                pl.BlockSpec((seq_len, HEAD_DIM), lambda h, i, order_ref: (0, h)),
            ],
        ),
        out_shape=[jax.ShapeDtypeStruct(q.shape, jnp.bfloat16), jax.ShapeDtypeStruct(k.shape, jnp.bfloat16)],
        compiler_params=params(16),
        cost_estimate=cost(9_000_000_000, 5_000_000),
    )(order, q, k, v, cos_t, sin_t)


def project_kernel(request, next_request, embeds_hbm, moved_hbm, gain_ref, wq_ref, wk_ref, wv_ref, q_ref, k_ref, v_ref, own_ref, *rest):
    a, b, s = lax.axis_index('a'), lax.axis_index('b'), lax.axis_index('stage')
    if next_request is not None:
        next_hbm, x, normed, sems, send_sem, recv_sem = rest
        passed = pltpu.make_async_remote_copy(
            src_ref=embeds_hbm.at[0, next_request], dst_ref=next_hbm, send_sem=send_sem, recv_sem=recv_sem,
            device_id={'stage': 1 - s}, device_id_type=pl.DeviceIdType.MESH)
    else:
        x, normed, sems = rest
    step = pl.program_id(0)
    last = pl.num_programs(0) - 1
    pieces = sems.shape[0]
    rows = x.shape[0] // pieces
    block = own_ref.shape[0] // 2

    @pl.when(step == 0)
    def _():
        def fetch(source, i):
            return pltpu.make_async_copy(source.at[pl.ds(i * rows, rows)], x.at[pl.ds(i * rows, rows)], sems.at[i])

        @pl.when(s == 0)
        def _():
            for i in range(pieces):
                fetch(embeds_hbm.at[0, request], i).start()

        @pl.when(s == 1)
        def _():
            for i in range(pieces):
                fetch(moved_hbm, i).start()

        if next_request is not None:
            barrier = pltpu.get_barrier_semaphore()
            pl.semaphore_signal(barrier, inc=1, device_id={'stage': 1 - s}, device_id_type=pl.DeviceIdType.MESH)
            pl.semaphore_wait(barrier, 1)

            @pl.when(s == 0)
            def _():
                passed.start()

        for i in range(pieces):
            fetch(moved_hbm, i).wait()
            normed[pl.ds(i * rows, rows), :] = normalised(x[pl.ds(i * rows, rows), :].astype(jnp.float32), gain_ref)
        for i, own in enumerate((2 * a + b, 4 + 2 * b + a)):
            own_ref[i * block:(i + 1) * block, :] = x[pl.ds(pl.multiple_of(own * block, 32), block), :]

    @pl.when(step < last)
    def _():
        q_ref[:] = matmul(normed[:], wq_ref[0]).astype(jnp.bfloat16)

    @pl.when(step == last)
    def _():
        k_ref[:] = matmul(normed[:], wk_ref[0]).astype(jnp.bfloat16)
        v_ref[:] = matmul(normed[:], wv_ref[0]).astype(jnp.bfloat16)
        if next_request is not None:
            @pl.when(s == 0)
            def _():
                passed.wait_send()

            @pl.when(s == 1)
            def _():
                passed.wait_recv()


def projections(embeds, moved, request, next_request, gain, w_query, w_key, w_value):
    seq_len, width = moved.shape
    q_width, kv_width = w_query.shape[2], w_key.shape[2]
    tile = 2 * kv_width
    q_steps = q_width // tile
    hbm = pl.BlockSpec(memory_space=pltpu.HBM)

    def first(shape):
        return pl.BlockSpec(shape, lambda j: (0,) * len(shape))

    def bf16(*shape):
        return jax.ShapeDtypeStruct(shape, jnp.bfloat16)

    out_specs = [
        pl.BlockSpec((seq_len, tile), lambda j: (0, jnp.minimum(j, q_steps - 1))),
        first((seq_len, kv_width)), first((seq_len, kv_width)), first((seq_len // 4, width))]
    out_shape = [bf16(seq_len, q_width), bf16(seq_len, kv_width), bf16(seq_len, kv_width), bf16(seq_len // 4, width)]
    scratch = [pltpu.VMEM((seq_len, width), jnp.bfloat16), pltpu.VMEM((seq_len, width), jnp.bfloat16), pltpu.SemaphoreType.DMA((4,))]
    extra = {}
    if next_request is not None:
        out_specs.append(hbm)
        out_shape.append(bf16(seq_len, width))
        scratch += [pltpu.SemaphoreType.DMA, pltpu.SemaphoreType.DMA]
        extra = dict(collective_id=1 + request, has_side_effects=True)
    return pl.pallas_call(
        functools.partial(project_kernel, request, next_request),
        grid=(q_steps + 1,),
        in_specs=[
            hbm, hbm, first((1, width)),
            pl.BlockSpec((1, width, tile), lambda j: (0, 0, jnp.minimum(j, q_steps - 1))),
            first((1, width, kv_width)), first((1, width, kv_width)),
        ],
        out_specs=out_specs,
        out_shape=out_shape,
        scratch_shapes=scratch,
        compiler_params=params(38, **extra),
        cost_estimate=cost(10_000_000_000, 30_000_000),
    )(embeds, moved, gain, w_query, w_key, w_value)


def gate_up_kernel(own_hbm, near_1_hbm, near_2_hbm, far_1_hbm, far_2_hbm, wg_ref, wu_ref, o_ref, rows, sems):
    block = near_1_hbm.shape[0]

    @pl.when(pl.program_id(0) == 0)
    def _():
        copies = []
        for i, (source, start) in enumerate((
                (own_hbm.at[pl.ds(0, block)], 0), (near_1_hbm, block), (far_1_hbm, 2 * block),
                (own_hbm.at[pl.ds(block, block)], 4 * block), (near_2_hbm, 5 * block), (far_2_hbm, 6 * block))):
            copies.append(pltpu.make_async_copy(source, rows.at[pl.ds(start, source.shape[0])], sems.at[i]))
            copies[-1].start()
        for copy in copies:
            copy.wait()

    gate = jnp.dot(rows[:], wg_ref[0], preferred_element_type=jnp.float32).astype(jnp.bfloat16).astype(jnp.float32)
    up = jnp.dot(rows[:], wu_ref[0], preferred_element_type=jnp.float32).astype(jnp.bfloat16).astype(jnp.float32)
    o_ref[:] = gated(gate, up)


def gate_up(own, near_1, near_2, far_1, far_2, w_gate, w_up, first, count, tile):
    block, width = near_1.shape
    hbm = pl.BlockSpec(memory_space=pltpu.HBM)
    weight = pl.BlockSpec((1, width, tile), lambda j: (0, 0, first + j))
    return pl.pallas_call(
        gate_up_kernel,
        grid=(count,),
        in_specs=[hbm] * 5 + [weight] * 2,
        out_specs=pl.BlockSpec((8 * block, tile), lambda j: (0, j)),
        out_shape=jax.ShapeDtypeStruct((8 * block, count * tile), jnp.bfloat16),
        scratch_shapes=[pltpu.VMEM((8 * block, width), jnp.bfloat16), pltpu.SemaphoreType.DMA((6,))],
        compiler_params=params(20),
        cost_estimate=cost(32 * block * width * count * tile, 4 * width * count * tile),
    )(own, near_1, near_2, far_1, far_2, w_gate, w_up)


def down_kernel(act_1_ref, act_2_ref, w_ref, *o_refs):
    cut = act_1_ref.shape[1]
    product = jnp.dot(act_1_ref[:], w_ref[0, :cut, :], preferred_element_type=jnp.float32)
    product = (product + jnp.dot(act_2_ref[:], w_ref[0, cut:, :], preferred_element_type=jnp.float32)).astype(jnp.bfloat16)
    rows = o_refs[0].shape[0]
    for i, o_ref in enumerate(o_refs):
        o_ref[:] = product[i * rows:(i + 1) * rows]


def down(act_1, act_2, w_down, tile):
    rows, depth = act_1.shape[0], w_down.shape[1]
    width = w_down.shape[2]
    return pl.pallas_call(
        down_kernel,
        grid=(width // tile,),
        in_specs=[pl.BlockSpec(act_1.shape, lambda j: (0, 0)), pl.BlockSpec(act_2.shape, lambda j: (0, 0)),
                  pl.BlockSpec((1, depth, tile), lambda j: (0, 0, j))],
        out_specs=[pl.BlockSpec((rows // 4, tile), lambda j: (0, j))] * 4,
        out_shape=[jax.ShapeDtypeStruct((rows // 4, width), jnp.bfloat16)] * 4,
        compiler_params=params(24),
        cost_estimate=cost(2 * rows * depth * width, 2 * depth * width),
    )(act_1, act_2, w_down)


def kv_kernel(part_ref, x_ref, gain_ref, cos_ref, sin_ref, *refs):
    mine, other, o_ref, normed = refs[:8], refs[8:16], refs[16], refs[17]
    depth, columns = mine[0].shape
    half = 2 * depth
    whole = normalised(x_ref[:].astype(jnp.float32), gain_ref)
    normed[0] = whole[:, :half]
    normed[1] = whole[:, half:]
    part = part_ref[0]
    for piece in range(4):
        product = jnp.dot(normed[part, :, :depth], mine[2 * piece][:], preferred_element_type=jnp.float32)
        product += jnp.dot(normed[part, :, depth:], mine[2 * piece + 1][:], preferred_element_type=jnp.float32)
        product += jnp.dot(normed[1 - part, :, :depth], other[2 * piece][:], preferred_element_type=jnp.float32)
        product += jnp.dot(normed[1 - part, :, depth:], other[2 * piece + 1][:], preferred_element_type=jnp.float32)
        rounded = product.astype(jnp.bfloat16)
        base = piece * columns
        for h in range(columns // 2 // HEAD_DIM):
            cols = slice(h * HEAD_DIM, (h + 1) * HEAD_DIM)
            o_ref[:, base + h * HEAD_DIM:base + (h + 1) * HEAD_DIM] = rotate(rounded[:, cols].astype(jnp.float32), cos_ref[:], sin_ref[:])
        o_ref[:, base + columns // 2:base + columns] = rounded[:, columns // 2:]


def keys_values(x, gain, mine, other, cos_rows, sin_rows, part):
    rows, _ = x.shape
    depth, columns = mine[0].shape
    vmem = pl.BlockSpec(memory_space=pltpu.VMEM)
    return pl.pallas_call(
        kv_kernel,
        in_specs=[pl.BlockSpec(memory_space=pltpu.SMEM)] + [vmem] * 20,
        out_specs=vmem,
        out_shape=jax.ShapeDtypeStruct((rows, 4 * columns), jnp.bfloat16),
        scratch_shapes=[pltpu.VMEM((2, rows, 2 * depth), jnp.bfloat16)],
        compiler_params=params(26),
        cost_estimate=cost(32 * rows * depth * columns, 32 * depth * columns),
    )(part, x, gain, cos_rows, sin_rows, *mine, *other)


def tail_kernel(kv_heads, x0_ref, x1_ref, x2_ref, kv0_ref, kv1_ref, kv2_ref, gain_a_ref, gain_m_ref, cos_ref, sin_ref,
                wq_hbm, wo_hbm, wg_hbm, wu_hbm, wd_hbm, o_ref,
                wq, wo, wg, wu, wd, x_src, x_all, q_src, q_all, pk_src, pk_all, mix, p_src, p_all, r_src, r_all,
                w_sem, x_send, x_recv, q_send, q_recv, pk_send, pk_recv, p_send, p_recv, r_send, r_recv):
    a, b, s = lax.axis_index('a'), lax.axis_index('b'), lax.axis_index('stage')
    me = 4 * b + 2 * a + s
    x_refs, kv_refs = (x0_ref, x1_ref, x2_ref), (kv0_ref, kv1_ref, kv2_ref)
    n_chunk = len(x_refs)
    n_rows = o_ref.shape[0]
    group = wq.shape[1] // HEAD_DIM
    eighth, wide = wq.shape[1], wg.shape[1]

    cuts = [
        (wq_hbm.at[1, :, pl.ds(pl.multiple_of(s * eighth, eighth), eighth)], wq),
        (wo_hbm.at[1, pl.ds(pl.multiple_of(s * eighth, eighth), eighth), :], wo),
        (wg_hbm.at[1, :, pl.ds(pl.multiple_of(s * wide, wide), wide)], wg),
        (wu_hbm.at[1, :, pl.ds(pl.multiple_of(s * wide, wide), wide)], wu),
        (wd_hbm.at[1, pl.ds(pl.multiple_of(s * wide, wide), wide), :], wd),
    ]
    fetches = [pltpu.make_async_copy(src, dst, w_sem.at[i]) for i, (src, dst) in enumerate(cuts)]
    for fetch in fetches:
        fetch.start()

    peers = []
    for d in range(1, 8):
        peer_b = 1 - b if d & 4 else b
        peer_a = 1 - a if d & 2 else a
        peer_s = 1 - s if d & 1 else s
        peers.append((4 * peer_b + 2 * peer_a + peer_s, {'b': peer_b, 'a': peer_a, 'stage': peer_s}))

    barrier = pltpu.get_barrier_semaphore()
    for _, where in peers:
        pl.semaphore_signal(barrier, inc=1, device_id=where, device_id_type=pl.DeviceIdType.MESH)
    pl.semaphore_wait(barrier, 7)

    def exchange(source_of, everyone, send, recv):
        copies = [
            pltpu.make_async_remote_copy(
                src_ref=source_of(peer), dst_ref=everyone.at[me], send_sem=send.at[i], recv_sem=recv.at[i],
                device_id=where, device_id_type=pl.DeviceIdType.MESH)
            for i, (peer, where) in enumerate(peers)]
        arrivals = [
            pltpu.make_async_remote_copy(
                src_ref=source_of(peer), dst_ref=everyone.at[peer], send_sem=send.at[i], recv_sem=recv.at[i],
                device_id=where, device_id_type=pl.DeviceIdType.MESH)
            for i, (peer, where) in enumerate(peers)]
        for copy in copies:
            copy.start()
        everyone[me] = source_of(me)[:]
        for arrival in arrivals:
            arrival.wait_recv()
        for copy in copies:
            copy.wait_send()

    row_index = lax.broadcasted_iota(jnp.int32, (n_rows, x0_ref.shape[1]), 0)
    rows = jnp.zeros((n_rows, x0_ref.shape[1]), jnp.float32)
    for c in range(n_chunk):
        last_row = x_refs[c][x_refs[c].shape[0] - 1:, :].astype(jnp.float32)
        rows = jnp.where(row_index == n_chunk * s + c, last_row, rows)
    x_src[:] = rows.astype(jnp.bfloat16)
    is_owner = a + b == 2

    def x_copy(i):
        return pltpu.make_async_remote_copy(
            src_ref=x_src, dst_ref=x_all.at[s], send_sem=x_send.at[i], recv_sem=x_recv.at[s],
            device_id=peers[i][1], device_id_type=pl.DeviceIdType.MESH)

    @pl.when(is_owner)
    def _():
        for i in range(7):
            x_copy(i).start()
        x_all[s] = x_src[:]

    for o in range(2):
        @pl.when(me != 6 + o)
        def _(o=o):
            pltpu.make_async_remote_copy(
                src_ref=x_src, dst_ref=x_all.at[o], send_sem=x_send.at[0], recv_sem=x_recv.at[o],
                device_id=peers[0][1], device_id_type=pl.DeviceIdType.MESH).wait_recv()

    @pl.when(is_owner)
    def _():
        for i in range(7):
            x_copy(i).wait_send()

    last = x_all[0].astype(jnp.float32) + x_all[1].astype(jnp.float32)
    fetches[0].wait()
    q = jnp.dot(normalised(last, gain_a_ref), wq[:], preferred_element_type=jnp.float32)
    q_src[:] = q.astype(jnp.bfloat16).astype(jnp.float32)
    exchange(lambda peer: q_src, q_all, q_send, q_recv)

    kv_width = kv_heads * HEAD_DIM
    for piece in range(4):
        head_b = 1 - b if piece & 2 else b
        head_a = 1 - a if piece & 1 else a
        for h in range(kv_heads):
            head = (2 * head_b + head_a) * kv_heads + h
            low = 2 * piece * kv_width + h * HEAD_DIM
            for c in range(n_chunk):
                q_row = q_all[head, pl.ds(n_chunk * s + c, 1), :]
                q_heads = jnp.concatenate([q_row[:, g * HEAD_DIM:(g + 1) * HEAD_DIM] for g in range(group)])
                q_heads = rotate(q_heads, cos_ref[:], sin_ref[:])
                k = kv_refs[c][:, low:low + HEAD_DIM]
                v = kv_refs[c][:, low + kv_width:low + kv_width + HEAD_DIM]
                scores = lax.dot_general(q_heads, k, (((1,), (1,)), ((), ())), preferred_element_type=jnp.float32) * HEAD_DIM ** -0.5
                top = jnp.max(scores, axis=-1, keepdims=True)
                probs = jnp.exp(scores - top)
                total = jnp.sum(probs, axis=-1, keepdims=True)
                pk_src[head, c, :, :HEAD_DIM] = jnp.dot(probs.astype(jnp.bfloat16), v, preferred_element_type=jnp.float32)
                pk_src[head, c, :, HEAD_DIM:2 * HEAD_DIM] = jnp.broadcast_to(top, (group, HEAD_DIM))
                pk_src[head, c, :, 2 * HEAD_DIM:] = jnp.broadcast_to(total, (group, HEAD_DIM))
    exchange(lambda peer: pk_src.at[peer], pk_all, pk_send, pk_recv)

    mix[:] = jnp.zeros_like(mix)
    for stage in range(2):
        for c in range(n_chunk):
            found = [pk_all[2 * i + stage, c] for i in range(4)]
            top = found[0][:, HEAD_DIM:2 * HEAD_DIM]
            for part in found[1:]:
                top = jnp.maximum(top, part[:, HEAD_DIM:2 * HEAD_DIM])
            value, total = jnp.zeros_like(top), jnp.zeros_like(top)
            for part in found:
                scale = jnp.exp(part[:, HEAD_DIM:2 * HEAD_DIM] - top)
                value += part[:, :HEAD_DIM] * scale
                total += part[:, 2 * HEAD_DIM:] * scale
            value = value / total
            for g in range(group):
                mix[n_chunk * stage + c:n_chunk * stage + c + 1, g * HEAD_DIM:(g + 1) * HEAD_DIM] = value[g:g + 1, :]

    def summed(everyone):
        total = everyone[0].astype(jnp.float32)
        for i in range(1, 8):
            total += everyone[i].astype(jnp.float32)
        return total.astype(jnp.bfloat16).astype(jnp.float32)

    fetches[1].wait()
    p_src[:] = jnp.dot(mix[:].astype(jnp.bfloat16), wo[:], preferred_element_type=jnp.float32).astype(jnp.bfloat16)
    exchange(lambda peer: p_src, p_all, p_send, p_recv)
    last = (last + summed(p_all)).astype(jnp.bfloat16).astype(jnp.float32)
    normed = normalised(last, gain_m_ref)
    fetches[2].wait()
    gate = jnp.dot(normed, wg[:], preferred_element_type=jnp.float32).astype(jnp.bfloat16).astype(jnp.float32)
    fetches[3].wait()
    up = jnp.dot(normed, wu[:], preferred_element_type=jnp.float32).astype(jnp.bfloat16).astype(jnp.float32)
    act = gated(gate, up)
    fetches[4].wait()
    r_src[:] = jnp.dot(act, wd[:], preferred_element_type=jnp.float32).astype(jnp.bfloat16)
    exchange(lambda peer: r_src, r_all, r_send, r_recv)
    o_ref[:] = (last + summed(r_all)).astype(jnp.bfloat16)


def last_rows(finals, kvs, gain_a, gain_m, cos_row, sin_row, w_query, w_out, w_gate, w_up, w_down, kv_heads):
    width = finals[0].shape[1]
    eighth = w_query.shape[2] // 2
    wide = w_gate.shape[2] // 2
    group = eighth // HEAD_DIM
    n_rows = 8
    n_chunk = len(finals)
    vmem = pl.BlockSpec(memory_space=pltpu.VMEM)
    last_block = pl.BlockSpec((n_rows, width), lambda i: (finals[0].shape[0] // n_rows - 1, 0))

    def full(value):
        return pl.BlockSpec(value.shape, lambda i: (0,) * value.ndim)

    seven = pltpu.SemaphoreType.DMA((7,))
    return pl.pallas_call(
        functools.partial(tail_kernel, kv_heads),
        grid=(1,),
        in_specs=[last_block] * n_chunk + [full(kv) for kv in kvs] + [full(v) for v in (gain_a, gain_m, cos_row, sin_row)]
        + [pl.BlockSpec(memory_space=pl.ANY)] * 5,
        out_specs=pl.BlockSpec((n_rows, width), lambda i: (0, 0)),
        out_shape=jax.ShapeDtypeStruct((n_rows, width), jnp.bfloat16),
        scratch_shapes=[
            pltpu.VMEM((width, eighth), jnp.bfloat16),
            pltpu.VMEM((eighth, width), jnp.bfloat16),
            pltpu.VMEM((width, wide), jnp.bfloat16),
            pltpu.VMEM((width, wide), jnp.bfloat16),
            pltpu.VMEM((wide, width), jnp.bfloat16),
            pltpu.VMEM((n_rows, width), jnp.bfloat16),
            pltpu.VMEM((2, n_rows, width), jnp.bfloat16),
            pltpu.VMEM((n_rows, eighth), jnp.float32),
            pltpu.VMEM((8, n_rows, eighth), jnp.float32),
            pltpu.VMEM((8, n_chunk, group, 3 * HEAD_DIM), jnp.float32),
            pltpu.VMEM((8, n_chunk, group, 3 * HEAD_DIM), jnp.float32),
            pltpu.VMEM((n_rows, eighth), jnp.float32),
            pltpu.VMEM((n_rows, width), jnp.bfloat16),
            pltpu.VMEM((8, n_rows, width), jnp.bfloat16),
            pltpu.VMEM((n_rows, width), jnp.bfloat16),
            pltpu.VMEM((8, n_rows, width), jnp.bfloat16),
            pltpu.SemaphoreType.DMA((5,)),
            seven, pltpu.SemaphoreType.DMA((2,)), seven, seven, seven, seven, seven, seven, seven, seven,
        ],
        compiler_params=params(63, collective_id=0, has_side_effects=True),
        cost_estimate=cost(9_000_000_000, 60_000_000),
    )(*finals, *kvs, gain_a, gain_m, cos_row, sin_row, w_query, w_out, w_gate, w_up, w_down)


def write_heads(k_ref, v_ref, low, high):
    rows, kv2 = low.shape
    for ref, start in ((k_ref, 0), (v_ref, kv2 // 2)):
        heads = jnp.concatenate([low[:, start:start + kv2 // 2], high[:, start:start + kv2 // 2]], axis=1)
        ref[0, 0, 0] = heads.reshape(rows, kv2 // HEAD_DIM, HEAD_DIM)


def first_cut_kernel(where_ref, near_ref, far_ref, k_ref, v_ref):
    own_low = where_ref[0] == 0
    near, far = near_ref[0], far_ref[0]
    write_heads(k_ref, v_ref, jnp.where(own_low, near, far), jnp.where(own_low, far, near))


def first_cut(near, far, where):
    n_chunk, seq_len, columns = near.shape
    rows = seq_len // 2
    heads = columns // HEAD_DIM
    source = pl.BlockSpec((1, rows, columns), lambda c, j, where_ref: (c, j, 0))
    target = pl.BlockSpec((1, 1, 1, rows, heads, HEAD_DIM), lambda c, j, where_ref: (0, 0, c, j, 0, 0))
    return pl.pallas_call(
        first_cut_kernel,
        grid_spec=pltpu.PrefetchScalarGridSpec(num_scalar_prefetch=1, grid=(n_chunk, 2), in_specs=[source] * 2, out_specs=[target] * 2),
        out_shape=[jax.ShapeDtypeStruct((1, 2, n_chunk, seq_len, heads, HEAD_DIM), jnp.bfloat16)] * 2,
        compiler_params=params(16),
        cost_estimate=cost(1_000_000_000, 19_000_000),
    )(where, near, far)


def second_cut_kernel(where_ref, near_ref, far_ref, k_in, v_in, k_ref, v_ref):
    columns = near_ref.shape[-1] // 2

    def put(source):
        mine, other = source[:, :columns], source[:, columns:]
        own_low = where_ref[0] + pl.program_id(0) - 2 * where_ref[0] * pl.program_id(0) == 0
        write_heads(k_ref, v_ref, jnp.where(own_low, mine, other), jnp.where(own_low, other, mine))

    @pl.when(pl.program_id(0) == 0)
    def _():
        put(near_ref[0])

    @pl.when(pl.program_id(0) == 1)
    def _():
        put(far_ref[0])


def second_cut(near, far, where, k_cache, v_cache, request):
    _, rows, columns = near.shape
    block = rows // 2
    heads = columns // 2 // HEAD_DIM

    def place(i, j, half, where_ref):
        along_x = where_ref[0] + i - 2 * where_ref[0] * i
        along_y = where_ref[1] + j - 2 * where_ref[1] * j
        return 0, 1, request, (1 - half) * (2 * along_x + along_y) + half * (4 + 2 * along_y + along_x), 0, 0

    source = pl.BlockSpec((1, block, columns), lambda i, j, half, where_ref: (j, half, 0))
    target = pl.BlockSpec((1, 1, 1, block, heads, HEAD_DIM), place)
    whole = pl.BlockSpec(memory_space=pl.ANY)
    return pl.pallas_call(
        second_cut_kernel,
        grid_spec=pltpu.PrefetchScalarGridSpec(
            num_scalar_prefetch=1, grid=(2, 2, 2), in_specs=[source] * 2 + [whole] * 2, out_specs=[target] * 2),
        out_shape=[jax.ShapeDtypeStruct(k_cache.shape, jnp.bfloat16)] * 2,
        input_output_aliases={3: 0, 4: 1},
        compiler_params=params(16),
        cost_estimate=cost(300_000_000, 5_000_000),
    )(where, near, far, k_cache, v_cache)


def solution(mesh):
    tp_axes = ('b', 'a')
    weight_cols = P(None, None, tp_axes)
    weight_rows = P(None, tp_axes, None)
    in_specs = (P('stage', 'dp', None, None), P(), weight_cols, weight_cols, weight_cols, weight_rows, P(), weight_cols, weight_cols, weight_rows)
    cache_spec = P('stage', None, ('dp', 'a'), None, 'b', None)
    out_specs = (cache_spec, cache_spec, P('stage', ('dp', 'a'), None))

    def over_x(value):
        return lax.ppermute(value, 'a', SWAP)

    def over_y(value):
        return lax.ppermute(value, 'b', SWAP)

    def across(value):
        return lax.ppermute(value, 'stage', SWAP)

    def hold(values, *after):
        return lax.optimization_barrier((values, after))[0]

    def stage_program(embeds, attn_gain, w_query, w_key, w_value, w_out, mlp_gain, w_gate, w_up, w_down):
        a, b, s = lax.axis_index('a'), lax.axis_index('b'), lax.axis_index('stage')
        n_req, seq_len, width = embeds.shape[1:]
        n_chunk = n_req // 2
        block = seq_len // 8
        kv_width = w_key.shape[2]
        kv_heads = kv_width // HEAD_DIM
        kv2 = 2 * kv_width
        half_rows = seq_len // 2
        half_width = width // 2
        cos_t, sin_t = rope_tables(seq_len)
        chip = 2 * b + a
        part = s.astype(jnp.int32).reshape(1)
        where = jnp.stack([a, b]).astype(jnp.int32)

        fours = jnp.arange(4, dtype=jnp.int32)
        order = jnp.concatenate([jnp.bitwise_xor(fours, 2 * a + b), 4 + jnp.bitwise_xor(fours, chip)]).astype(jnp.int32)

        def own_rows(value):
            return jnp.concatenate([
                lax.dynamic_slice_in_dim(value, block * (2 * a + b), block, 0),
                lax.dynamic_slice_in_dim(value, half_rows + block * chip, block, 0)])

        def quarters(part_sum):
            return [part_sum[2 * i * block:2 * (i + 1) * block] for i in range(4)]

        def send_parts(parts):
            return parts[1], parts[3]

        def send_wide(sends):
            return over_x(sends[0]), over_y(sends[1])

        def add_wide(parts, got):
            return add_rounded(parts[0], got[0]), add_rounded(parts[2], got[1])

        def send_narrow(sums):
            return over_y(sums[0][block:]), over_x(sums[1][block:])

        def add_narrow(residual, sums, got):
            kept = jnp.concatenate([sums[0][:block], sums[1][:block]])
            return add_rounded(residual, add_rounded(kept, jnp.concatenate(got)))

        def gather_near(own):
            return over_y(own[:block]), over_x(own[block:])

        def join_near(own, got):
            return jnp.concatenate([own[:block], got[0]]), jnp.concatenate([own[block:], got[1]])

        def gather_far(near):
            return over_x(near[0]), over_y(near[1])

        def take(value):
            return lax.ppermute(value, 'stage', [(0, 1)])

        moved0 = take(embeds[0, n_chunk])

        quarter_width = width // 4

        def w_block(half, lower):
            rows = half * half_width + lower * quarter_width
            return jnp.concatenate([lax.dynamic_slice_in_dim(w[1], rows, quarter_width, 0) for w in (w_key, w_value)], axis=1)

        w_top, w_bottom = hold((w_block(s, 0), w_block(s, 1)), embeds[0, n_chunk, :8, :128])
        top_y, bottom_x = over_y(w_top), over_x(w_bottom)
        top_x, bottom_y = over_x(w_top), over_y(w_bottom)

        def project(moved, request):
            following = n_chunk + request + 1 if request + 1 < n_chunk else None
            q, k, v, own, *passed = projections(embeds, moved, request, following, attn_gain[:1], w_query, w_key, w_value)
            return (q, k, v), own, passed

        def attend(qkv):
            mix, k_rot = attention(*qkv, cos_t, sin_t, order)
            return mix, jnp.concatenate([k_rot, qkv[2]], axis=1)

        def out_of(mix):
            return quarters(matmul(mix, w_out[0]).astype(jnp.bfloat16))

        mlp_tile = w_key.shape[2]
        n_tiles = w_gate.shape[2] // mlp_tile
        first_tiles = n_tiles // 2

        def act_of(h, got, far, second):
            start, count = (first_tiles, n_tiles - first_tiles) if second else (0, first_tiles)
            return gate_up(h, got[0], got[1], far[0], far[1], w_gate, w_up, start, count, mlp_tile)

        def down_of(act_1, act_2):
            return down(act_1, act_2, w_down, 2 * mlp_tile)

        own_cos, own_sin = own_rows(cos_t), own_rows(sin_t)

        qkv0, own_x0, (moved1,) = project(moved0, 0)
        top_d, bottom_d = over_x(hold(top_y, qkv0)), over_y(hold(bottom_x, qkv0))
        mix0, kv0_0 = attend(qkv0)
        p0 = out_of(mix0)
        send = send_parts(p0)
        wide0 = send_wide(send)

        qkv1, own_x1, (moved2,) = project(hold(moved1, send), 1)
        sums0 = add_wide(p0, hold(wide0, qkv1))
        narrow0 = send_narrow(sums0)
        mix1, kv0_1 = attend(hold(qkv1, sums0))
        own1_0 = add_narrow(own_x0, sums0, hold(narrow0, mix1))
        h0 = rms_norm(own1_0, mlp_gain[0])
        near_got0 = gather_near(h0)
        p1 = out_of(hold(mix1, h0))
        send = send_parts(p1)
        wide1 = send_wide(send)
        near0 = join_near(h0, hold(near_got0, send))
        far0 = gather_far(near0)

        qkv2, own_x2, _ = project(hold(moved2, near0), 2)
        mix2, kv0_2 = attend(qkv2)
        sums1 = add_wide(p1, hold(wide1, mix2))
        narrow1 = send_narrow(sums1)
        p2 = out_of(hold(mix2, sums1))
        send = send_parts(p2)
        wide2 = send_wide(send)

        rows = (h0, near_got0, hold(far0, send))
        gate = act_of(*rows, False)
        own1_1 = add_narrow(own_x1, sums1, hold(narrow1, gate))
        h1 = rms_norm(own1_1, mlp_gain[0])
        near_got1 = gather_near(h1)
        act = act_of(*hold(rows, h1), True)
        near1 = join_near(h1, hold(near_got1, act))
        far1 = gather_far(near1)
        sums2 = add_wide(p2, hold(wide2, near1))
        narrow2 = send_narrow(sums2)
        d0 = down_of(gate, hold(act, sums2))
        send = send_parts(d0)
        wide0 = send_wide(send)

        fetched = hold((top_x, bottom_x, top_y, bottom_y, top_d, bottom_d), send)
        w_mine = [w_top, w_bottom] + list(fetched)
        w_other = [w_block(1 - s, 0), w_block(1 - s, 1)] + [across(piece) for piece in fetched]

        rows = (h1, near_got1, hold(far1, send))
        gate = act_of(*rows, False)
        own1_2 = add_narrow(own_x2, sums2, hold(narrow2, gate))
        h2 = rms_norm(own1_2, mlp_gain[0])
        near_got2 = gather_near(h2)
        act = act_of(*hold(rows, h2), True)
        near2 = join_near(h2, hold(near_got2, act))
        far2 = gather_far(near2)
        sums0 = add_wide(d0, hold(wide0, near2))
        narrow0 = send_narrow(sums0)
        d1 = down_of(gate, hold(act, sums0))
        send = send_parts(d1)
        wide1 = send_wide(send)

        def keys_values_of(final):
            return keys_values(final, attn_gain[1:2], w_mine, w_other, own_cos, own_sin, part)

        def to_decode(value):
            return lax.ppermute(value, ('a', 'stage'), FROM_NEAR), lax.ppermute(value, ('a', 'stage'), FROM_FAR)

        def along_y(kv, *after):
            return over_y(hold(kv[:, 2 * kv2:], *after))

        def to_decode_rows(kv, got):
            return to_decode(jnp.stack([kv[:, :2 * kv2], got]))

        rows = (h2, near_got2, hold(far2, send))
        gate = act_of(*rows, False)
        final0 = add_narrow(own1_0, sums0, hold(narrow0, gate))
        kv1_0 = keys_values_of(final0)
        got_0 = along_y(kv1_0)
        cut0 = to_decode(hold(jnp.stack([kv0_0, kv0_1, kv0_2]), kv1_0))
        act = act_of(*hold(rows, kv1_0), True)
        sums1 = add_wide(d1, hold(wide1, act))
        narrow1 = send_narrow(sums1)
        cut1_0 = to_decode_rows(kv1_0, hold(got_0, sums1))
        d2 = down_of(gate, hold(act, sums1))
        send = send_parts(d2)
        wide2 = send_wide(send)
        final1 = add_narrow(own1_1, sums1, hold(narrow1, send))
        kv1_1 = keys_values_of(final1)
        got_1 = along_y(kv1_1)
        k_cache, v_cache = first_cut(*hold(cut0, kv1_1), where)
        sums2 = add_wide(d2, hold(wide2, k_cache))
        narrow2 = send_narrow(sums2)
        k_cache, v_cache = second_cut(*hold(cut1_0, sums2), where, k_cache, v_cache, 0)
        final2 = add_narrow(own1_2, sums2, hold(narrow2, k_cache))
        kv1_2 = keys_values_of(final2)
        got_2 = along_y(kv1_2)
        cut1_1 = to_decode_rows(kv1_1, hold(got_1, kv1_2))
        cut1_2 = to_decode_rows(kv1_2, got_2)

        last = last_rows(
            (final0, final1, final2), (kv1_0, kv1_1, hold(kv1_2, got_2)), attn_gain[1:2], mlp_gain[1:2],
            cos_t[-1:], sin_t[-1:], w_query, w_out, w_gate, w_up, w_down, kv_heads)
        last_out = lax.dynamic_slice_in_dim(last, a * n_chunk, n_chunk, 0)
        last_out = jnp.where(s == 1, last_out, jnp.zeros_like(last_out))

        for c, cut in ((1, cut1_1), (2, cut1_2)):
            k_cache, v_cache = second_cut(*hold(cut, last), where, k_cache, v_cache, c)
        return k_cache, v_cache, last_out[None]

    return jax.shard_map(stage_program, mesh=mesh, in_specs=in_specs, out_specs=out_specs, check_vma=False)
```
